128 devices in a mesh: model: 16 (over z, y), fsdp: 8 (over x, core).
Axes of the slice: x: 4, y: 4, z: 4, core: 2. Of those that a mesh axis runs over, the one named last changes fastest.
Arguments:
- tok_ids: int32 [8, 2048], P('fsdp')
- tok_labels: int32 [8, 2048], P('fsdp')
- emb_table: bfloat16 [32128, 768], P(('model', 'fsdp'))
- w_gate: bfloat16 [768, 2048], P('fsdp')
- w_up: bfloat16 [768, 2048], P('fsdp')
- w_down: bfloat16 [2048, 768], P('fsdp')
- gain_in: float32 [768], replicated
- gain_out: float32 [768], replicated
Outputs:
- output 1: float32 [], replicated
- output 2: float32 [32128, 768], P(('model', 'fsdp'))
- output 3: float32 [768, 2048], P('fsdp')
- output 4: float32 [768, 2048], P('fsdp')
- output 5: float32 [2048, 768], P('fsdp')
All inputs are finite; a program needn't handle non-finite values.
Results may differ from the reference program's by a relative error of at most 0.00822918.
Values are sent between devices in bfloat16 or wider.
A program may use at most 1 GiB of HBM per device.

```python
import jax
import jax.numpy as jnp
from jax import lax

V = 32128
D = 768
F = 2048
BATCH = 8
SEQ = 2048
HEAD_BLOCK = 64
EPS = 1e-6


def draw_tokens(base_key):
    id_key, label_key = jax.random.split(base_key)
    tok_ids = jax.random.randint(id_key, (BATCH, SEQ), 0, V, dtype=jnp.int32)
    tok_ids = tok_ids.at[0, 0].set(0).at[BATCH - 1, SEQ - 1].set(V - 1)
    tok_labels = jax.random.randint(label_key, (BATCH, SEQ), 0, V, dtype=jnp.int32)
    tok_labels = tok_labels.at[0, 0].set(V - 1).at[BATCH - 1, SEQ - 1].set(0)
    return tok_ids, tok_labels


def setup_inputs(seed: int = 0) -> dict:
    rng_keys = jax.random.split(jax.random.key(seed), 7)
    tok_ids, tok_labels = draw_tokens(rng_keys[0])
    emb_table = (jax.random.normal(rng_keys[1], (V, D), jnp.float32) * D ** -0.5).astype(jnp.bfloat16)
    w_gate = (jax.random.normal(rng_keys[2], (D, F), jnp.float32) * D ** -0.5).astype(jnp.bfloat16)
    w_up = (jax.random.normal(rng_keys[3], (D, F), jnp.float32) * D ** -0.5).astype(jnp.bfloat16)
    w_down = (jax.random.normal(rng_keys[4], (F, D), jnp.float32) * (2.0 * (F * D) ** -0.5)).astype(jnp.bfloat16)
    gain_in = jax.random.uniform(rng_keys[5], (D,), jnp.float32, 0.5, 1.5)
    gain_out = jax.random.uniform(rng_keys[6], (D,), jnp.float32, 0.5, 1.5)
    return {"tok_ids": tok_ids, "tok_labels": tok_labels, "emb_table": emb_table, "w_gate": w_gate, "w_up": w_up, "w_down": w_down, "gain_in": gain_in, "gain_out": gain_out}


def rms_scale(values, gain_vec):
    mean_sq = jnp.mean(values * values, axis=-1, keepdims=True)
    return values * lax.rsqrt(mean_sq + EPS) * gain_vec


def reference(tok_ids, tok_labels, emb_table, w_gate, w_up, w_down, gain_in, gain_out):
    num_tokens = BATCH * SEQ
    flat_ids = tok_ids.reshape(num_tokens)
    flat_labels = tok_labels.reshape(num_tokens)
    x_emb = emb_table[flat_ids].astype(jnp.float32)
    normed_in, norm_in_back = jax.vjp(lambda values: rms_scale(values, gain_in), x_emb)
    normed_bf = normed_in.astype(jnp.bfloat16)
    gate_f = jnp.dot(normed_bf, w_gate, preferred_element_type=jnp.float32).astype(jnp.bfloat16).astype(jnp.float32)
    up_f = jnp.dot(normed_bf, w_up, preferred_element_type=jnp.float32).astype(jnp.bfloat16).astype(jnp.float32)
    gate_sig = jax.nn.sigmoid(gate_f)
    silu_gate = gate_f * gate_sig
    act_bf = (silu_gate * up_f).astype(jnp.bfloat16)
    mlp_out = jnp.dot(act_bf, w_down, preferred_element_type=jnp.float32).astype(jnp.bfloat16)
    h_res = x_emb + mlp_out.astype(jnp.float32)
    hn_f, norm_out_back = jax.vjp(lambda values: rms_scale(values, gain_out), h_res)
    hn_bf = hn_f.astype(jnp.bfloat16)
    num_blocks = num_tokens // HEAD_BLOCK
    hn_blocks = hn_bf.reshape(num_blocks, HEAD_BLOCK, D)
    label_blocks = flat_labels.reshape(num_blocks, HEAD_BLOCK)

    def head_step(d_head, block_in):
        hn_blk, label_blk = block_in
        logits = jnp.dot(hn_blk, emb_table.T, preferred_element_type=jnp.float32)
        row_max = jnp.max(logits, axis=-1, keepdims=True)
        exp_shift = jnp.exp(logits - row_max)
        sum_exp = jnp.sum(exp_shift, axis=-1, keepdims=True)
        onehot = lax.broadcasted_iota(jnp.int32, logits.shape, 1) == label_blk[:, None]
        label_logit = jnp.sum(jnp.where(onehot, logits, 0.0), axis=-1)
        tok_loss = row_max[:, 0] + jnp.log(sum_exp[:, 0]) - label_logit
        soft_probs = exp_shift / sum_exp
        d_logits = (jnp.where(onehot, soft_probs - 1.0, soft_probs) / num_tokens).astype(jnp.bfloat16)
        d_head = d_head + jnp.dot(d_logits.T, hn_blk, preferred_element_type=jnp.float32)
        d_hn = jnp.dot(d_logits, emb_table, preferred_element_type=jnp.float32)
        return d_head, (tok_loss, d_hn)

    d_head, (tok_losses, d_hn_blocks) = lax.scan(head_step, jnp.zeros((V, D), jnp.float32), (hn_blocks, label_blocks))
    loss = jnp.sum(tok_losses) / num_tokens
    d_hn = d_hn_blocks.reshape(num_tokens, D)
    d_hidden = norm_out_back(d_hn)[0]
    d_mlp = d_hidden.astype(jnp.bfloat16)
    d_act = jnp.dot(d_mlp, w_down.T, preferred_element_type=jnp.float32)
    grad_down = jnp.dot(act_bf.T, d_mlp, preferred_element_type=jnp.float32)
    d_gate = (d_act * up_f * (gate_sig * (1.0 + gate_f * (1.0 - gate_sig)))).astype(jnp.bfloat16)
    d_up = (d_act * silu_gate).astype(jnp.bfloat16)
    grad_gate = jnp.dot(normed_bf.T, d_gate, preferred_element_type=jnp.float32)
    grad_up = jnp.dot(normed_bf.T, d_up, preferred_element_type=jnp.float32)
    d_normed = jnp.dot(d_gate, w_gate.T, preferred_element_type=jnp.float32) + jnp.dot(d_up, w_up.T, preferred_element_type=jnp.float32)
    d_x = d_hidden + norm_in_back(d_normed)[0]
    d_in = jax.ops.segment_sum(d_x, flat_ids, num_segments=V)
    grad_table = d_head + d_in
    return (loss, grad_table, grad_gate, grad_up, grad_down)
```

```python
import functools

import jax
import jax.numpy as jnp
from jax import lax
from jax.experimental import pallas as pl
from jax.experimental.pallas import tpu as pltpu
from jax.sharding import PartitionSpec as P

EPS = 1e-6
F32 = jnp.float32
BF16 = jnp.bfloat16


def rms_scale(values, gain_vec):
    mean_sq = jnp.mean(values * values, axis=-1, keepdims=True)
    return values * lax.rsqrt(mean_sq + EPS) * gain_vec


def dot(spec, lhs, rhs):
    return jnp.einsum(spec, lhs, rhs, preferred_element_type=F32)


def add_rows_kernel(cap, count_ref, row_ref, add_ref, base_ref, out_ref):
    out_ref[...] = base_ref[...]

    def chunk(c, carry):
        def step(j, carry):
            row = row_ref[c * cap + j]
            out_ref[pl.ds(row, 1), :] += add_ref[pl.ds(c * cap + j, 1), :]
            return carry

        return lax.fori_loop(0, count_ref[c], step, carry)

    lax.fori_loop(0, count_ref.shape[0], chunk, 0)


def add_rows(base, rows, row_ids, counts, cap):
    vmem = pl.BlockSpec(memory_space=pltpu.VMEM)
    smem = pl.BlockSpec(memory_space=pltpu.SMEM)
    return pl.pallas_call(
        functools.partial(add_rows_kernel, cap),
        out_shape=jax.ShapeDtypeStruct(base.shape, base.dtype),
        in_specs=[smem, smem, vmem, vmem],
        out_specs=vmem,
        cost_estimate=pl.CostEstimate(flops=20_000_000, bytes_accessed=20_000_000, transcendentals=0),
    )(counts, row_ids, rows, base)


def solution(mesh):
    n_model, n_fsdp = mesh.shape["model"], mesh.shape["fsdp"]
    tok_spec = P("fsdp", None)
    row_spec = P(("model", "fsdp"), None)
    weight_spec = P("fsdp", None)

    def device_step(tok_ids, tok_labels, table_shard, gate_shard, up_shard, down_shard, gain_in, gain_out):
        me = lax.axis_index("model")
        group = tok_ids.shape[0] * tok_ids.shape[1]
        num_tokens = group * n_fsdp
        part = group // n_model
        rows, width = table_shard.shape
        pad_rows = -(-rows // 16) * 16
        block = rows * n_fsdp
        pad_block = pad_rows * n_fsdp
        hidden = gate_shard.shape[1]
        wg_rows, wd_rows = gate_shard.shape[0], down_shard.shape[0]
        sl = wd_rows // n_model
        fs = sl * n_fsdp

        table = lax.all_gather(jnp.pad(table_shard, ((0, pad_rows - rows), (0, 0))), "fsdp", axis=0, tiled=True)
        gate_all = gate_shard.reshape(wg_rows, n_fsdp, n_model, sl)
        up_all = up_shard.reshape(wg_rows, n_fsdp, n_model, sl)
        gate_sl = lax.dynamic_index_in_dim(gate_all, me, 2, keepdims=False).reshape(wg_rows, fs)
        up_sl = lax.dynamic_index_in_dim(up_all, me, 2, keepdims=False).reshape(wg_rows, fs)
        down_sl = lax.dynamic_slice_in_dim(down_shard, me * sl, sl, 0).reshape(wg_rows, fs)
        w_cat = jnp.concatenate([gate_sl, up_sl, down_sl], 0)
        w_cat = lax.all_gather(w_cat, ("model", "fsdp"), axis=0, tiled=True)
        w_cat = w_cat.reshape(n_model, n_fsdp, 3, wg_rows, fs)
        w_gate = w_cat[:, :, 0].reshape(n_model, width, fs)
        w_up = w_cat[:, :, 1].reshape(n_model, width, fs)
        w_down = w_cat[:, :, 2].reshape(n_model, fs, width)

        cap = part // 4
        ids = tok_ids.reshape(group)
        blk = (ids // block).reshape(n_model, part)
        loc = ids - me * block
        loc = (loc + (pad_rows - rows) * (loc // rows)).reshape(n_model, part)
        p_iota = jnp.arange(part, dtype=jnp.int32)
        m_iota = jnp.arange(n_model, dtype=jnp.int32)
        same = (blk[:, :, None] == blk[:, None, :]) & (p_iota[None, None, :] < p_iota[None, :, None])
        rank = jnp.sum(same.astype(jnp.int32), axis=2)
        cnt = jnp.sum((blk[:, :, None] == m_iota).astype(jnp.int32), axis=1)
        own_cnt = jnp.sum((blk == me).astype(jnp.int32), axis=1)
        rounds = (lax.pmax(jnp.max(cnt), "fsdp") + cap - 1) // cap
        j_iota = jnp.arange(cap, dtype=jnp.int32)
        my_blk = lax.dynamic_index_in_dim(blk, me, 0, keepdims=False)
        my_rank = lax.dynamic_index_in_dim(rank, me, 0, keepdims=False)

        def slots(k):
            hit = (blk[:, None, :] == me) & (rank[:, None, :] == (j_iota + k * cap)[None, :, None])
            return jnp.sum(jnp.where(hit, loc[:, None, :], 0), axis=2).reshape(n_model * cap)

        def pick(k):
            place = my_blk * cap + my_rank - k * cap
            place = jnp.where((my_rank >= k * cap) & (my_rank < (k + 1) * cap), place, -1)
            return place[:, None] == jnp.arange(n_model * cap, dtype=jnp.int32)[None, :]

        def fetch(k):
            got = lax.all_to_all(jnp.take(table, slots(k), axis=0), "model", 0, 0, tiled=True)
            return dot("ij,jd->id", pick(k).astype(BF16), got)

        def give(k, d_x, base):
            send = jnp.einsum("ij,id->jd", pick(k).astype(F32), d_x, precision=lax.Precision.HIGHEST, preferred_element_type=F32)
            got = lax.all_to_all(send, "model", 0, 0, tiled=True)
            return add_rows(base, got, slots(k), jnp.clip(own_cnt - k * cap, 0, cap), cap)

        x_emb = fetch(0)
        x_emb = lax.while_loop(lambda c: c[0] < rounds, lambda c: (c[0] + 1, c[1] + fetch(c[0])), (jnp.int32(1), x_emb))[1]

        normed_in, norm_in_back = jax.vjp(lambda values: rms_scale(values, gain_in), x_emb)
        a_bf = normed_in.astype(BF16)
        a_all = lax.all_gather(a_bf, "model", axis=0, tiled=True)
        gate_f = dot("td,mdf->tmf", a_bf, w_gate).astype(BF16).astype(F32)
        up_f = dot("td,mdf->tmf", a_bf, w_up).astype(BF16).astype(F32)
        gate_sig = jax.nn.sigmoid(gate_f)
        silu_gate = gate_f * gate_sig
        act_bf = (silu_gate * up_f).astype(BF16)
        mlp_out = dot("tmf,mfd->td", act_bf, w_down).astype(BF16)
        h_res = x_emb + mlp_out.astype(F32)
        hn_f, norm_out_back = jax.vjp(lambda values: rms_scale(values, gain_out), h_res)
        hn_bf = lax.all_gather(hn_f.astype(BF16), "model", axis=0, tiled=True)

        labels = tok_labels.reshape(group)
        lab = labels - me * block
        lab_in = (lab >= 0) & (lab < block)
        lab = jnp.where(lab_in, lab + (pad_rows - rows) * (lab // rows), -1)
        col = lax.broadcasted_iota(jnp.int32, (group, pad_block), 1)
        logits = dot("td,vd->tv", hn_bf, table)
        logits = jnp.where(col % pad_rows < rows, logits, -jnp.inf)
        loc_max = jnp.max(logits, axis=-1)
        loc_sum = jnp.sum(jnp.exp(logits - loc_max[:, None]), axis=-1)
        onehot = col == lab[:, None]
        loc_lab = jnp.sum(jnp.where(onehot, logits, 0.0), axis=-1)
        stats = lax.all_gather(jnp.stack([loc_max, loc_sum, loc_lab]), "model", axis=0)
        row_max = jnp.max(stats[:, 0], axis=0)
        sum_exp = jnp.sum(stats[:, 1] * jnp.exp(stats[:, 0] - row_max), axis=0)
        tok_loss = row_max + jnp.log(sum_exp) - jnp.sum(stats[:, 2], axis=0)
        loss_part = jnp.sum(tok_loss)
        soft = jnp.exp(logits - row_max[:, None]) / sum_exp[:, None]
        d_logits = (jnp.where(onehot, soft - 1.0, soft) / num_tokens).astype(BF16)
        d_hn = lax.psum_scatter(dot("tv,vd->td", d_logits, table), "model", scatter_dimension=0, tiled=True)
        d_head = dot("tv,td->vd", d_logits, hn_bf)

        d_hidden = norm_out_back(d_hn)[0]
        d_mlp = d_hidden.astype(BF16)
        dm_all = lax.all_gather(d_mlp, "model", axis=0, tiled=True)
        d_act = dot("td,mfd->tmf", d_mlp, w_down)
        silu_back = gate_sig * (1.0 + gate_f * (1.0 - gate_sig))
        d_gate = (d_act * up_f * silu_back).astype(BF16)
        d_up = (d_act * silu_gate).astype(BF16)
        d_normed = dot("tmf,mdf->td", d_gate, w_gate) + dot("tmf,mdf->td", d_up, w_up)
        d_x = d_hidden + norm_in_back(d_normed)[0]
        grad_block = give(0, d_x, d_head)
        grad_block = lax.while_loop(lambda c: c[0] < rounds, lambda c: (c[0] + 1, give(c[0], d_x, c[1])), (jnp.int32(1), grad_block))[1]
        grad_table = lax.psum_scatter(grad_block, "fsdp", scatter_dimension=0, tiled=True)[:rows]

        wg_s = lax.dynamic_index_in_dim(w_gate, me, 0, keepdims=False)
        wu_s = lax.dynamic_index_in_dim(w_up, me, 0, keepdims=False)
        wd_s = lax.dynamic_index_in_dim(w_down, me, 0, keepdims=False)
        gs = dot("td,df->tf", a_all, wg_s).astype(BF16).astype(F32)
        us = dot("td,df->tf", a_all, wu_s).astype(BF16).astype(F32)
        sig_s = jax.nn.sigmoid(gs)
        silu_s = gs * sig_s
        act_s = (silu_s * us).astype(BF16)
        d_act_s = dot("td,fd->tf", dm_all, wd_s)
        d_gate_s = (d_act_s * us * (sig_s * (1.0 + gs * (1.0 - sig_s)))).astype(BF16)
        d_up_s = (d_act_s * silu_s).astype(BF16)
        gg = dot("td,tf->df", a_all, d_gate_s).reshape(n_fsdp, wg_rows, fs)
        gu = dot("td,tf->df", a_all, d_up_s).reshape(n_fsdp, wg_rows, fs)
        gd = dot("tf,td->fd", act_s, dm_all).reshape(n_fsdp, wg_rows, fs)
        gl = jnp.full((n_fsdp, 8, fs), loss_part)
        cat = jnp.concatenate([gg, gu, gd, gl], 1).reshape(-1, fs)
        cat = lax.psum_scatter(cat, "fsdp", scatter_dimension=0, tiled=True)
        loss = cat[3 * wg_rows, 0] / num_tokens
        cat = lax.all_gather(cat, "model", axis=0)[:, : 3 * wg_rows].reshape(n_model, 3, wg_rows, fs)
        grad_gate = cat[:, 0].reshape(n_model, wg_rows, n_fsdp, sl).transpose(1, 2, 0, 3).reshape(wg_rows, hidden)
        grad_up = cat[:, 1].reshape(n_model, wg_rows, n_fsdp, sl).transpose(1, 2, 0, 3).reshape(wg_rows, hidden)
        grad_down = cat[:, 2].reshape(wd_rows, width)
        return loss, grad_table, grad_gate, grad_up, grad_down

    return jax.shard_map(device_step, mesh=mesh, in_specs=(tok_spec, tok_spec, row_spec, weight_spec, weight_spec, weight_spec, P(), P()), out_specs=(P(), row_spec, weight_spec, weight_spec, weight_spec), check_vma=False)
```

```python
import functools

import jax
import jax.numpy as jnp
from jax import lax
from jax.experimental import pallas as pl
from jax.experimental.pallas import tpu as pltpu
from jax.sharding import PartitionSpec as P

EPS = 1e-6
F32 = jnp.float32
BF16 = jnp.bfloat16


def rms_scale(values, gain_vec):
    mean_sq = jnp.mean(values * values, axis=-1, keepdims=True)
    return values * lax.rsqrt(mean_sq + EPS) * gain_vec


def dot(spec, lhs, rhs):
    return jnp.einsum(spec, lhs, rhs, preferred_element_type=F32)


def add_rows_kernel(cap, count_ref, row_ref, add_ref, base_ref, out_ref):
    out_ref[...] = base_ref[...]

    def chunk(c, carry):
        def step(j, carry):
            row = row_ref[c * cap + j]
            out_ref[pl.ds(row, 1), :] += add_ref[pl.ds(c * cap + j, 1), :]
            return carry

        return lax.fori_loop(0, count_ref[c], step, carry)

    lax.fori_loop(0, count_ref.shape[0], chunk, 0)


def add_rows(base, rows, row_ids, counts, cap):
    vmem = pl.BlockSpec(memory_space=pltpu.VMEM)
    smem = pl.BlockSpec(memory_space=pltpu.SMEM)
    return pl.pallas_call(
        functools.partial(add_rows_kernel, cap),
        out_shape=jax.ShapeDtypeStruct(base.shape, base.dtype),
        in_specs=[smem, smem, vmem, vmem],
        out_specs=vmem,
        cost_estimate=pl.CostEstimate(flops=20_000_000, bytes_accessed=20_000_000, transcendentals=0),
    )(counts, row_ids, rows, base)


MODEL_SIDE = 4


def plane_coords():
    me = lax.axis_index("model")
    return me // MODEL_SIDE, me % MODEL_SIDE


def shifted(color, dim, delta):
    z, y = plane_coords()
    if (color == 0) == (dim == 0):
        y = (y + delta + MODEL_SIDE) % MODEL_SIDE
    else:
        z = (z + delta + MODEL_SIDE) % MODEL_SIDE
    return z, y


def shifted2(color, delta1, delta2):
    z, y = plane_coords()
    if color == 0:
        return (z + delta2 + MODEL_SIDE) % MODEL_SIDE, (y + delta1 + MODEL_SIDE) % MODEL_SIDE
    return (z + delta1 + MODEL_SIDE) % MODEL_SIDE, (y + delta2 + MODEL_SIDE) % MODEL_SIDE


def plane_device(color, dim, delta):
    z, y = shifted(color, dim, delta)
    return {"model": z * MODEL_SIDE + y}


def greet_plane():
    barrier = pltpu.get_barrier_semaphore()
    for dim in (0, 1):
        for delta in (1, -1):
            pl.semaphore_signal(barrier, inc=1, device_id=plane_device(0, dim, delta), device_id_type=pl.DeviceIdType.MESH)
    pl.semaphore_wait(barrier, 4)


GATHER_OPS = 22


def plane_gather_kernel(x_ref, out_ref, send_sem, recv_sem):
    z, y = plane_coords()
    greet_plane()
    started = {}

    def send(color, op, dim, delta, src, dst):
        copy = pltpu.make_async_remote_copy(
            src_ref=src, dst_ref=dst, send_sem=send_sem.at[color, op], recv_sem=recv_sem.at[color, op],
            device_id=plane_device(color, dim, delta), device_id_type=pl.DeviceIdType.MESH)
        copy.start()
        started[color, op] = copy

    def got(color, op):
        started[color, op].wait_recv()

    def block(color, d1, d2):
        zz, yy = shifted2(color, d1, d2)
        return out_ref.at[zz, yy, color]

    def half(color, d1, d2, h):
        zz, yy = shifted2(color, d1, d2)
        return out_ref.at[zz, yy, color, h]

    colors = (0, 1)
    for c in colors:
        for k, delta in enumerate((1, -1)):
            send(c, k, 0, delta, x_ref.at[c], block(c, 0, 0))
        for k, delta in enumerate((1, -1)):
            send(c, 4 + k, 1, delta, x_ref.at[c], block(c, 0, 0))
    out_ref[z, y] = x_ref[...]
    for k in (0, 1):
        side = -1 if k == 0 else 1
        for c in colors:
            got(c, k)
            send(c, 2 + k, 0, -side, half(c, side, 0, k), half(c, side, 0, k))
            for j, delta in enumerate((1, -1)):
                send(c, 6 + 2 * k + j, 1, delta, block(c, side, 0), block(c, side, 0))
    for k in (0, 1):
        side = -1 if k == 0 else 1
        for c in colors:
            got(c, 4 + k)
            send(c, 14 + k, 1, -side, half(c, 0, side, k), half(c, 0, side, k))
    for k in (0, 1):
        for c in colors:
            got(c, 2 + k)
            for j, delta in enumerate((1, -1)):
                send(c, 10 + 2 * k + j, 1, delta, half(c, 2, 0, k), half(c, 2, 0, k))
    for s, col in ((0, -1), (1, 1)):
        for k in (0, 1):
            side = -1 if k == 0 else 1
            for c in colors:
                got(c, 6 + 2 * s + k)
                send(c, 16 + 2 * s + k, 1, -side, half(c, col, side, k), half(c, col, side, k))
    for k in (0, 1):
        side = -1 if k == 0 else 1
        for c in colors:
            got(c, 10 + 2 * k + k)
            send(c, 20 + k, 1, -side, half(c, 2, side, k), half(c, 2, side, k))
    for c in colors:
        got(c, 11)
        got(c, 12)
        for op in range(14, GATHER_OPS):
            got(c, op)
    for copy in started.values():
        copy.wait_send()


def plane_gather(x, collective_id):
    rows, width = x.shape
    quarter = rows // 4
    vmem = pl.BlockSpec(memory_space=pltpu.VMEM)
    out = pl.pallas_call(
        plane_gather_kernel,
        out_shape=jax.ShapeDtypeStruct((MODEL_SIDE, MODEL_SIDE, 2, 2, quarter, width), x.dtype),
        in_specs=[vmem],
        out_specs=vmem,
        scratch_shapes=[pltpu.SemaphoreType.DMA((2, GATHER_OPS)), pltpu.SemaphoreType.DMA((2, GATHER_OPS))],
        compiler_params=pltpu.CompilerParams(collective_id=collective_id, has_side_effects=True),
        cost_estimate=pl.CostEstimate(flops=40_000_000_000, bytes_accessed=4_000_000, transcendentals=0),
    )(x.reshape(2, 2, quarter, width))
    return out.reshape(MODEL_SIDE * MODEL_SIDE, rows, width)


def plane_scatter_kernel(x_ref, out_ref, far1, near1, relay1, sum1, far2, near2, relay2, send_sem, recv_sem):
    greet_plane()
    started = []

    def send(color, op, dim, delta, src, dst):
        copy = pltpu.make_async_remote_copy(
            src_ref=src, dst_ref=dst, send_sem=send_sem.at[color, op], recv_sem=recv_sem.at[color, op],
            device_id=plane_device(color, dim, delta), device_id_type=pl.DeviceIdType.MESH)
        copy.start()
        started.append(copy)
        return copy

    def mine(color, d1, d2, h):
        zz, yy = shifted2(color, d1, d2)
        return x_ref.at[zz, yy, color, h]

    colors = (0, 1)
    order = (2, 1, -1, 0)
    sides = ((0, 1), (1, -1))
    copies = {}
    for n, d2 in enumerate(order):
        for c in colors:
            for k, delta in sides:
                copies[c, n, k] = send(c, 2 * n + k, 0, delta, mine(c, 2, d2, k), far1.at[c, n, k])
    for n, d2 in enumerate(order):
        for c in colors:
            for k, delta in sides:
                copies[c, n, 2 + k] = send(c, 8 + 2 * n + k, 0, delta, mine(c, delta, d2, 1 - k), near1.at[c, n, k, 0])
        for c in colors:
            for k, delta in sides:
                copies[c, n, k].wait_recv()
                relay1[c, n, k] = far1[c, n, k] + mine(c, delta, d2, k)[...]
                copies[c, n, 4 + k] = send(c, 16 + 2 * n + k, 0, delta, relay1.at[c, n, k], near1.at[c, n, k, 1])
    for n, d2 in enumerate(order):
        for c in colors:
            for k in (2, 3, 4, 5):
                copies[c, n, k].wait_recv()
            for h in (0, 1):
                sum1[c, n, h] = mine(c, 0, d2, h)[...] + near1[c, n, h, 1] + near1[c, n, 1 - h, 0]
            if n == 0:
                for k, delta in sides:
                    copies[c, "far", k] = send(c, 24 + k, 1, delta, sum1.at[c, 0, k], far2.at[c, k])
            if n in (1, 2):
                k, delta = sides[n - 1]
                copies[c, "raw", k] = send(c, 26 + k, 1, delta, sum1.at[c, n, 1 - k], near2.at[c, k, 0])
                copies[c, "far", k].wait_recv()
                relay2[c, k] = far2[c, k] + sum1[c, n, k]
                copies[c, "sum", k] = send(c, 28 + k, 1, delta, relay2.at[c, k], near2.at[c, k, 1])
    for c in colors:
        for k in (0, 1):
            copies[c, "raw", k].wait_recv()
            copies[c, "sum", k].wait_recv()
        for h in (0, 1):
            out_ref[c, h] = sum1[c, 3, h] + near2[c, h, 1] + near2[c, 1 - h, 0]
    for copy in started:
        copy.wait_send()


def plane_scatter(x, collective_id):
    _, rows, width = x.shape
    quarter = rows // 4
    vmem = pl.BlockSpec(memory_space=pltpu.VMEM)
    piece = (quarter, width)
    out = pl.pallas_call(
        plane_scatter_kernel,
        out_shape=jax.ShapeDtypeStruct((2, 2, quarter, width), F32),
        in_specs=[vmem],
        out_specs=vmem,
        scratch_shapes=[
            pltpu.VMEM((2, 4, 2) + piece, F32),
            pltpu.VMEM((2, 4, 2, 2) + piece, F32),
            pltpu.VMEM((2, 4, 2) + piece, F32),
            pltpu.VMEM((2, 4, 2) + piece, F32),
            pltpu.VMEM((2, 2) + piece, F32),
            pltpu.VMEM((2, 2, 2) + piece, F32),
            pltpu.VMEM((2, 2) + piece, F32),
            pltpu.SemaphoreType.DMA((2, 30)),
            pltpu.SemaphoreType.DMA((2, 30)),
        ],
        compiler_params=pltpu.CompilerParams(collective_id=collective_id, has_side_effects=True),
        cost_estimate=pl.CostEstimate(flops=60_000_000_000, bytes_accessed=8_000_000, transcendentals=0),
    )(x.reshape(MODEL_SIDE, MODEL_SIDE, 2, 2, quarter, width))
    return out.reshape(rows, width)


def solution(mesh):
    n_model, n_fsdp = mesh.shape["model"], mesh.shape["fsdp"]
    tok_spec = P("fsdp", None)
    row_spec = P(("model", "fsdp"), None)
    weight_spec = P("fsdp", None)

    def device_step(tok_ids, tok_labels, table_shard, gate_shard, up_shard, down_shard, gain_in, gain_out):
        me = lax.axis_index("model")
        group = tok_ids.shape[0] * tok_ids.shape[1]
        num_tokens = group * n_fsdp
        part = group // n_model
        rows, width = table_shard.shape
        pad_rows = -(-rows // 16) * 16
        block = rows * n_fsdp
        pad_block = pad_rows * n_fsdp
        hidden = gate_shard.shape[1]
        wg_rows, wd_rows = gate_shard.shape[0], down_shard.shape[0]
        sl = wd_rows // n_model
        fs = sl * n_fsdp

        table = lax.all_gather(jnp.pad(table_shard, ((0, pad_rows - rows), (0, 0))), "fsdp", axis=0, tiled=True)
        gate_all = gate_shard.reshape(wg_rows, n_fsdp, n_model, sl)
        up_all = up_shard.reshape(wg_rows, n_fsdp, n_model, sl)
        gate_sl = lax.dynamic_index_in_dim(gate_all, me, 2, keepdims=False).reshape(wg_rows, fs)
        up_sl = lax.dynamic_index_in_dim(up_all, me, 2, keepdims=False).reshape(wg_rows, fs)
        down_sl = lax.dynamic_slice_in_dim(down_shard, me * sl, sl, 0).reshape(wg_rows, fs)
        w_cat = jnp.concatenate([gate_sl, up_sl, down_sl], 0)
        w_cat = lax.all_gather(w_cat, ("model", "fsdp"), axis=0, tiled=True)
        w_cat = w_cat.reshape(n_model, n_fsdp, 3, wg_rows, fs)
        w_gate = w_cat[:, :, 0].reshape(n_model, width, fs)
        w_up = w_cat[:, :, 1].reshape(n_model, width, fs)
        w_down = w_cat[:, :, 2].reshape(n_model, fs, width)

        cap = part // 4
        ids = tok_ids.reshape(group)
        blk = (ids // block).reshape(n_model, part)
        loc = ids - me * block
        loc = (loc + (pad_rows - rows) * (loc // rows)).reshape(n_model, part)
        p_iota = jnp.arange(part, dtype=jnp.int32)
        m_iota = jnp.arange(n_model, dtype=jnp.int32)
        same = (blk[:, :, None] == blk[:, None, :]) & (p_iota[None, None, :] < p_iota[None, :, None])
        rank = jnp.sum(same.astype(jnp.int32), axis=2)
        cnt = jnp.sum((blk[:, :, None] == m_iota).astype(jnp.int32), axis=1)
        own_cnt = jnp.sum((blk == me).astype(jnp.int32), axis=1)
        rounds = (lax.pmax(jnp.max(cnt), "fsdp") + cap - 1) // cap
        j_iota = jnp.arange(cap, dtype=jnp.int32)
        my_blk = lax.dynamic_index_in_dim(blk, me, 0, keepdims=False)
        my_rank = lax.dynamic_index_in_dim(rank, me, 0, keepdims=False)

        def slots(k):
            hit = (blk[:, None, :] == me) & (rank[:, None, :] == (j_iota + k * cap)[None, :, None])
            return jnp.sum(jnp.where(hit, loc[:, None, :], 0), axis=2).reshape(n_model * cap)

        def pick(k):
            place = my_blk * cap + my_rank - k * cap
            place = jnp.where((my_rank >= k * cap) & (my_rank < (k + 1) * cap), place, -1)
            return place[:, None] == jnp.arange(n_model * cap, dtype=jnp.int32)[None, :]

        def fetch(k):
            got = lax.all_to_all(jnp.take(table, slots(k), axis=0), "model", 0, 0, tiled=True)
            return dot("ij,jd->id", pick(k).astype(BF16), got)

        def give(k, d_x, base):
            send = jnp.einsum("ij,id->jd", pick(k).astype(F32), d_x, precision=lax.Precision.HIGHEST, preferred_element_type=F32)
            got = lax.all_to_all(send, "model", 0, 0, tiled=True)
            return add_rows(base, got, slots(k), jnp.clip(own_cnt - k * cap, 0, cap), cap)

        x_emb = fetch(0)
        x_emb = lax.while_loop(lambda c: c[0] < rounds, lambda c: (c[0] + 1, c[1] + fetch(c[0])), (jnp.int32(1), x_emb))[1]

        normed_in, norm_in_back = jax.vjp(lambda values: rms_scale(values, gain_in), x_emb)
        a_bf = normed_in.astype(BF16)
        a_all = lax.all_gather(a_bf, "model", axis=0, tiled=True)
        gate_f = dot("td,mdf->tmf", a_bf, w_gate).astype(BF16).astype(F32)
        up_f = dot("td,mdf->tmf", a_bf, w_up).astype(BF16).astype(F32)
        gate_sig = jax.nn.sigmoid(gate_f)
        silu_gate = gate_f * gate_sig
        act_bf = (silu_gate * up_f).astype(BF16)
        mlp_out = dot("tmf,mfd->td", act_bf, w_down).astype(BF16)
        h_res = x_emb + mlp_out.astype(F32)
        hn_f, norm_out_back = jax.vjp(lambda values: rms_scale(values, gain_out), h_res)
        hn_bf = plane_gather(hn_f.astype(BF16), 1).reshape(group, width)

        labels = tok_labels.reshape(group)
        lab = labels - me * block
        lab_in = (lab >= 0) & (lab < block)
        lab = jnp.where(lab_in, lab + (pad_rows - rows) * (lab // rows), -1)
        col = lax.broadcasted_iota(jnp.int32, (group, pad_block), 1)
        logits = dot("td,vd->tv", hn_bf, table)
        logits = jnp.where(col % pad_rows < rows, logits, -jnp.inf)
        loc_max = jnp.max(logits, axis=-1)
        loc_sum = jnp.sum(jnp.exp(logits - loc_max[:, None]), axis=-1)
        onehot = col == lab[:, None]
        loc_lab = jnp.sum(jnp.where(onehot, logits, 0.0), axis=-1)
        stats = jnp.stack([loc_max, loc_sum, loc_lab, loc_lab]).reshape(-1, 128)
        stats = plane_gather(stats, 2).reshape(n_model, 4, group)
        row_max = jnp.max(stats[:, 0], axis=0)
        sum_exp = jnp.sum(stats[:, 1] * jnp.exp(stats[:, 0] - row_max), axis=0)
        tok_loss = row_max + jnp.log(sum_exp) - jnp.sum(stats[:, 2], axis=0)
        loss_part = jnp.sum(tok_loss)
        soft = jnp.exp(logits - row_max[:, None]) / sum_exp[:, None]
        d_logits = (jnp.where(onehot, soft - 1.0, soft) / num_tokens).astype(BF16)
        d_hn = plane_scatter(dot("tv,vd->td", d_logits, table).reshape(n_model, part, width), 3)
        d_head = dot("tv,td->vd", d_logits, hn_bf)

        d_hidden = norm_out_back(d_hn)[0]
        d_mlp = d_hidden.astype(BF16)
        dm_all = plane_gather(d_mlp, 4).reshape(group, width)
        d_act = dot("td,mfd->tmf", d_mlp, w_down)
        silu_back = gate_sig * (1.0 + gate_f * (1.0 - gate_sig))
        d_gate = (d_act * up_f * silu_back).astype(BF16)
        d_up = (d_act * silu_gate).astype(BF16)
        d_normed = dot("tmf,mdf->td", d_gate, w_gate) + dot("tmf,mdf->td", d_up, w_up)
        d_x = d_hidden + norm_in_back(d_normed)[0]
        grad_block = give(0, d_x, d_head)
        grad_block = lax.while_loop(lambda c: c[0] < rounds, lambda c: (c[0] + 1, give(c[0], d_x, c[1])), (jnp.int32(1), grad_block))[1]
        grad_table = lax.psum_scatter(grad_block, "fsdp", scatter_dimension=0, tiled=True)[:rows]

        wg_s = lax.dynamic_index_in_dim(w_gate, me, 0, keepdims=False)
        wu_s = lax.dynamic_index_in_dim(w_up, me, 0, keepdims=False)
        wd_s = lax.dynamic_index_in_dim(w_down, me, 0, keepdims=False)
        gs = dot("td,df->tf", a_all, wg_s).astype(BF16).astype(F32)
        us = dot("td,df->tf", a_all, wu_s).astype(BF16).astype(F32)
        sig_s = jax.nn.sigmoid(gs)
        silu_s = gs * sig_s
        act_s = (silu_s * us).astype(BF16)
        d_act_s = dot("td,fd->tf", dm_all, wd_s)
        d_gate_s = (d_act_s * us * (sig_s * (1.0 + gs * (1.0 - sig_s)))).astype(BF16)
        d_up_s = (d_act_s * silu_s).astype(BF16)
        gg = dot("td,tf->df", a_all, d_gate_s).reshape(n_fsdp, wg_rows, fs)
        gu = dot("td,tf->df", a_all, d_up_s).reshape(n_fsdp, wg_rows, fs)
        gd = dot("tf,td->fd", act_s, dm_all).reshape(n_fsdp, wg_rows, fs)
        gl = jnp.full((n_fsdp, 16, fs), loss_part)
        cat = jnp.concatenate([gg, gu, gd, gl], 1).reshape(-1, fs)
        cat = lax.psum_scatter(cat, "fsdp", scatter_dimension=0, tiled=True)
        loss = cat[3 * wg_rows, 0] / num_tokens
        cat = plane_gather(cat[: 3 * wg_rows], 5).reshape(n_model, 3, wg_rows, fs)
        grad_gate = cat[:, 0].reshape(n_model, wg_rows, n_fsdp, sl).transpose(1, 2, 0, 3).reshape(wg_rows, hidden)
        grad_up = cat[:, 1].reshape(n_model, wg_rows, n_fsdp, sl).transpose(1, 2, 0, 3).reshape(wg_rows, hidden)
        grad_down = cat[:, 2].reshape(wd_rows, width)
        return loss, grad_table, grad_gate, grad_up, grad_down

    return jax.shard_map(device_step, mesh=mesh, in_specs=(tok_spec, tok_spec, row_spec, weight_spec, weight_spec, weight_spec, P(), P()), out_specs=(P(), row_spec, weight_spec, weight_spec, weight_spec), check_vma=False)
```

```python
import functools

import jax
import jax.numpy as jnp
from jax import lax
from jax.experimental import pallas as pl
from jax.experimental.pallas import tpu as pltpu
from jax.sharding import PartitionSpec as P

EPS = 1e-6
F32 = jnp.float32
BF16 = jnp.bfloat16


def rms_scale(values, gain_vec):
    mean_sq = jnp.mean(values * values, axis=-1, keepdims=True)
    return values * lax.rsqrt(mean_sq + EPS) * gain_vec


def dot(spec, lhs, rhs):
    return jnp.einsum(spec, lhs, rhs, preferred_element_type=F32)


def add_rows_kernel(cap, count_ref, row_ref, add_ref, base_ref, out_ref):
    out_ref[...] = base_ref[...]

    def chunk(c, carry):
        def step(j, carry):
            row = row_ref[c * cap + j]
            out_ref[pl.ds(row, 1), :] += add_ref[pl.ds(c * cap + j, 1), :]
            return carry

        return lax.fori_loop(0, count_ref[c], step, carry)

    lax.fori_loop(0, count_ref.shape[0], chunk, 0)


def add_rows(base, rows, row_ids, counts, cap):
    vmem = pl.BlockSpec(memory_space=pltpu.VMEM)
    smem = pl.BlockSpec(memory_space=pltpu.SMEM)
    return pl.pallas_call(
        functools.partial(add_rows_kernel, cap),
        out_shape=jax.ShapeDtypeStruct(base.shape, base.dtype),
        in_specs=[smem, smem, vmem, vmem],
        out_specs=vmem,
        cost_estimate=pl.CostEstimate(flops=1_500_000_000, bytes_accessed=20_000_000, transcendentals=0),
    )(counts, row_ids, rows, base)


MODEL_SIDE = 4


def plane_coords():
    me = lax.axis_index("model")
    return me // MODEL_SIDE, me % MODEL_SIDE


def shifted(color, dim, delta):
    z, y = plane_coords()
    if (color == 0) == (dim == 0):
        y = (y + delta + MODEL_SIDE) % MODEL_SIDE
    else:
        z = (z + delta + MODEL_SIDE) % MODEL_SIDE
    return z, y


def shifted2(color, delta1, delta2):
    z, y = plane_coords()
    if color == 0:
        return (z + delta2 + MODEL_SIDE) % MODEL_SIDE, (y + delta1 + MODEL_SIDE) % MODEL_SIDE
    return (z + delta1 + MODEL_SIDE) % MODEL_SIDE, (y + delta2 + MODEL_SIDE) % MODEL_SIDE


def plane_device(color, dim, delta):
    z, y = shifted(color, dim, delta)
    return {"model": z * MODEL_SIDE + y}


def greet_plane():
    barrier = pltpu.get_barrier_semaphore()
    for dim in (0, 1):
        for delta in (1, -1):
            pl.semaphore_signal(barrier, inc=1, device_id=plane_device(0, dim, delta), device_id_type=pl.DeviceIdType.MESH)
    pl.semaphore_wait(barrier, 4)


GATHER_OPS = 22


def plane_gather_kernel(x_ref, out_ref, send_sem, recv_sem):
    z, y = plane_coords()
    greet_plane()
    started = {}

    def send(color, op, dim, delta, src, dst):
        copy = pltpu.make_async_remote_copy(
            src_ref=src, dst_ref=dst, send_sem=send_sem.at[color, op], recv_sem=recv_sem.at[color, op],
            device_id=plane_device(color, dim, delta), device_id_type=pl.DeviceIdType.MESH)
        copy.start()
        started[color, op] = copy

    def got(color, op):
        started[color, op].wait_recv()

    def block(color, d1, d2):
        zz, yy = shifted2(color, d1, d2)
        return out_ref.at[zz, yy, color]

    def half(color, d1, d2, h):
        zz, yy = shifted2(color, d1, d2)
        return out_ref.at[zz, yy, color, h]

    colors = (0, 1)
    for c in colors:
        for k, delta in enumerate((1, -1)):
            send(c, k, 0, delta, x_ref.at[c], block(c, 0, 0))
        for k, delta in enumerate((1, -1)):
            send(c, 4 + k, 1, delta, x_ref.at[c], block(c, 0, 0))
    out_ref[z, y] = x_ref[...]
    for k in (0, 1):
        side = -1 if k == 0 else 1
        for c in colors:
            got(c, k)
            send(c, 2 + k, 0, -side, half(c, side, 0, k), half(c, side, 0, k))
            for j, delta in enumerate((1, -1)):
                send(c, 6 + 2 * k + j, 1, delta, block(c, side, 0), block(c, side, 0))
    for k in (0, 1):
        side = -1 if k == 0 else 1
        for c in colors:
            got(c, 4 + k)
            send(c, 14 + k, 1, -side, half(c, 0, side, k), half(c, 0, side, k))
    for k in (0, 1):
        for c in colors:
            got(c, 2 + k)
            for j, delta in enumerate((1, -1)):
                send(c, 10 + 2 * k + j, 1, delta, half(c, 2, 0, k), half(c, 2, 0, k))
    for s, col in ((0, -1), (1, 1)):
        for k in (0, 1):
            side = -1 if k == 0 else 1
            for c in colors:
                got(c, 6 + 2 * s + k)
                send(c, 16 + 2 * s + k, 1, -side, half(c, col, side, k), half(c, col, side, k))
    for k in (0, 1):
        side = -1 if k == 0 else 1
        for c in colors:
            got(c, 10 + 2 * k + k)
            send(c, 20 + k, 1, -side, half(c, 2, side, k), half(c, 2, side, k))
    for c in colors:
        got(c, 11)
        got(c, 12)
        for op in range(14, GATHER_OPS):
            got(c, op)
    for copy in started.values():
        copy.wait_send()


def plane_gather(x, collective_id):
    rows, width = x.shape
    quarter = rows // 4
    vmem = pl.BlockSpec(memory_space=pltpu.VMEM)
    out = pl.pallas_call(
        plane_gather_kernel,
        out_shape=jax.ShapeDtypeStruct((MODEL_SIDE, MODEL_SIDE, 2, 2, quarter, width), x.dtype),
        in_specs=[vmem],
        out_specs=vmem,
        scratch_shapes=[pltpu.SemaphoreType.DMA((2, GATHER_OPS)), pltpu.SemaphoreType.DMA((2, GATHER_OPS))],
        compiler_params=pltpu.CompilerParams(collective_id=collective_id, has_side_effects=True),
        cost_estimate=pl.CostEstimate(flops=5_000_000_000, bytes_accessed=4_000_000, transcendentals=0),
    )(x.reshape(2, 2, quarter, width))
    return out.reshape(MODEL_SIDE * MODEL_SIDE, rows, width)


def plane_scatter_kernel(x_ref, dz_ref, hn_ref, out_ref, head_ref, far1, near1, relay1, sum1, far2, near2, relay2, dz_buf, hn_buf, head_buf, send_sem, recv_sem, dz_sem, hn_sem, head_sem):
    greet_plane()
    started = []
    hn_copy = pltpu.make_async_copy(hn_ref, hn_buf, hn_sem)
    n_blocks = dz_ref.shape[0]
    dz_copies = [pltpu.make_async_copy(dz_ref.at[i], dz_buf.at[i], dz_sem.at[i]) for i in range(n_blocks)]
    head_copies = []

    def head_block():
        i = len(head_copies)
        if i == 0:
            hn_copy.wait()
        dz_copies[i].wait()
        head_buf[i] = jnp.dot(dz_buf[i], hn_buf[...], preferred_element_type=F32)
        copy = pltpu.make_async_copy(head_buf.at[i], head_ref.at[i], head_sem.at[i])
        copy.start()
        head_copies.append(copy)


    def send(color, op, dim, delta, src, dst):
        copy = pltpu.make_async_remote_copy(
            src_ref=src, dst_ref=dst, send_sem=send_sem.at[color, op], recv_sem=recv_sem.at[color, op],
            device_id=plane_device(color, dim, delta), device_id_type=pl.DeviceIdType.MESH)
        copy.start()
        started.append(copy)
        return copy

    def mine(color, d1, d2, h):
        zz, yy = shifted2(color, d1, d2)
        return x_ref.at[zz, yy, color, h]

    colors = (0, 1)
    order = (2, 1, -1, 0)
    sides = ((0, 1), (1, -1))
    copies = {}
    for n, d2 in enumerate(order):
        for c in colors:
            for k, delta in sides:
                copies[c, n, k] = send(c, 2 * n + k, 0, delta, mine(c, 2, d2, k), far1.at[c, n, k])
    hn_copy.start()
    for copy in dz_copies:
        copy.start()
    for n, d2 in enumerate(order):
        for c in colors:
            for k, delta in sides:
                copies[c, n, 2 + k] = send(c, 8 + 2 * n + k, 0, delta, mine(c, delta, d2, 1 - k), near1.at[c, n, k, 0])
        for c in colors:
            for k, delta in sides:
                copies[c, n, k].wait_recv()
                relay1[c, n, k] = far1[c, n, k] + mine(c, delta, d2, k)[...]
                copies[c, n, 4 + k] = send(c, 16 + 2 * n + k, 0, delta, relay1.at[c, n, k], near1.at[c, n, k, 1])
        head_block()
    for n, d2 in enumerate(order):
        head_block()
        for c in colors:
            for k in (2, 3, 4, 5):
                copies[c, n, k].wait_recv()
            for h in (0, 1):
                sum1[c, n, h] = mine(c, 0, d2, h)[...] + near1[c, n, h, 1] + near1[c, n, 1 - h, 0]
            if n == 0:
                for k, delta in sides:
                    copies[c, "far", k] = send(c, 24 + k, 1, delta, sum1.at[c, 0, k], far2.at[c, k])
            if n in (1, 2):
                k, delta = sides[n - 1]
                copies[c, "raw", k] = send(c, 26 + k, 1, delta, sum1.at[c, n, 1 - k], near2.at[c, k, 0])
                copies[c, "far", k].wait_recv()
                relay2[c, k] = far2[c, k] + sum1[c, n, k]
                copies[c, "sum", k] = send(c, 28 + k, 1, delta, relay2.at[c, k], near2.at[c, k, 1])
    for c in colors:
        for k in (0, 1):
            copies[c, "raw", k].wait_recv()
            copies[c, "sum", k].wait_recv()
        for h in (0, 1):
            out_ref[c, h] = sum1[c, 3, h] + near2[c, h, 1] + near2[c, 1 - h, 0]
    while len(head_copies) < n_blocks:
        head_block()
    for copy in started:
        copy.wait_send()
    for copy in head_copies:
        copy.wait()


def plane_scatter(x, dz, hn, collective_id):
    _, rows, width = x.shape
    n_blocks = 8
    vocab, tokens = dz.shape
    block_rows = vocab // n_blocks
    any_space = pl.BlockSpec(memory_space=pl.ANY)
    quarter = rows // 4
    vmem = pl.BlockSpec(memory_space=pltpu.VMEM)
    piece = (quarter, width)
    out, head = pl.pallas_call(
        plane_scatter_kernel,
        out_shape=(jax.ShapeDtypeStruct((2, 2, quarter, width), F32), jax.ShapeDtypeStruct((n_blocks, block_rows, width), F32)),
        in_specs=[vmem, any_space, any_space],
        out_specs=(vmem, any_space),
        scratch_shapes=[
            pltpu.VMEM((2, 4, 2) + piece, F32),
            pltpu.VMEM((2, 4, 2, 2) + piece, F32),
            pltpu.VMEM((2, 4, 2) + piece, F32),
            pltpu.VMEM((2, 4, 2) + piece, F32),
            pltpu.VMEM((2, 2) + piece, F32),
            pltpu.VMEM((2, 2, 2) + piece, F32),
            pltpu.VMEM((2, 2) + piece, F32),
            pltpu.VMEM((n_blocks, block_rows, tokens), BF16),
            pltpu.VMEM((tokens, width), BF16),
            pltpu.VMEM((n_blocks, block_rows, width), F32),
            pltpu.SemaphoreType.DMA((2, 30)),
            pltpu.SemaphoreType.DMA((2, 30)),
            pltpu.SemaphoreType.DMA((n_blocks,)),
            pltpu.SemaphoreType.DMA(()),
            pltpu.SemaphoreType.DMA((n_blocks,)),
        ],
        compiler_params=pltpu.CompilerParams(collective_id=collective_id, has_side_effects=True),
        cost_estimate=pl.CostEstimate(flops=10_000_000_000, bytes_accessed=8_000_000, transcendentals=0),
    )(x.reshape(MODEL_SIDE, MODEL_SIDE, 2, 2, quarter, width), dz.reshape(n_blocks, block_rows, tokens), hn)
    return out.reshape(rows, width), head.reshape(vocab, width)


def stats_kernel(x_ref, out_ref, buf1, comb, buf2, send_sem, recv_sem):
    z, y = plane_coords()

    def peer(dim, d):
        zz, yy = (z, (y + d) % MODEL_SIDE) if dim == 0 else ((z + d) % MODEL_SIDE, y)
        return {"model": zz * MODEL_SIDE + yy}

    barrier = pltpu.get_barrier_semaphore()
    for dim in (0, 1):
        for d in (1, 2, 3):
            pl.semaphore_signal(barrier, inc=1, device_id=peer(dim, d), device_id_type=pl.DeviceIdType.MESH)
    pl.semaphore_wait(barrier, 6)

    def merged(buf):
        top = jnp.maximum(jnp.maximum(buf[0, 0], buf[1, 0]), jnp.maximum(buf[2, 0], buf[3, 0]))
        total = jnp.zeros_like(top)
        label = jnp.zeros_like(top)
        for k in range(MODEL_SIDE):
            total = total + buf[k, 1] * jnp.exp(buf[k, 0] - top)
            label = label + buf[k, 2]
        return top, total, label

    for dim, src, buf, place, dst in ((0, x_ref, buf1, y, comb), (1, comb, buf2, z, out_ref)):
        copies = []
        for d in (1, 2, 3):
            copy = pltpu.make_async_remote_copy(
                src_ref=src, dst_ref=buf.at[place], send_sem=send_sem.at[dim, d - 1], recv_sem=recv_sem.at[dim, d - 1],
                device_id=peer(dim, d), device_id_type=pl.DeviceIdType.MESH)
            copy.start()
            copies.append(copy)
        buf[place] = src[...]
        for copy in copies:
            copy.wait_recv()
        top, total, label = merged(buf)
        dst[0] = top
        dst[1] = total
        dst[2] = label
        for copy in copies:
            copy.wait_send()


def stats_exchange(stats, collective_id):
    rows = stats.shape[1] // 128
    vmem = pl.BlockSpec(memory_space=pltpu.VMEM)
    out = pl.pallas_call(
        stats_kernel,
        out_shape=jax.ShapeDtypeStruct((3, rows, 128), F32),
        in_specs=[vmem],
        out_specs=vmem,
        scratch_shapes=[
            pltpu.VMEM((MODEL_SIDE, 3, rows, 128), F32),
            pltpu.VMEM((3, rows, 128), F32),
            pltpu.VMEM((MODEL_SIDE, 3, rows, 128), F32),
            pltpu.SemaphoreType.DMA((2, 3)),
            pltpu.SemaphoreType.DMA((2, 3)),
        ],
        compiler_params=pltpu.CompilerParams(collective_id=collective_id, has_side_effects=True),
        cost_estimate=pl.CostEstimate(flops=2_500_000_000, bytes_accessed=400_000, transcendentals=0),
    )(stats.reshape(3, rows, 128))
    return out.reshape(3, rows * 128)


def weights_kernel(gu_ref, dn_ref, most_ref, gu_out, dn_out, most_out, send_sem, recv_sem, mate_send, mate_recv, most_send, most_recv):
    z, y = plane_coords()
    f = lax.axis_index("fsdp")
    x, core = f // 2, f % 2
    mesh_id = pl.DeviceIdType.MESH

    def x_peer(d):
        return {"fsdp": ((x + d) % 4) * 2 + core}

    mate = {"fsdp": x * 2 + 1 - core}
    barrier = pltpu.get_barrier_semaphore()
    for dim in (0, 1):
        for delta in (1, -1):
            pl.semaphore_signal(barrier, inc=1, device_id=plane_device(0, dim, delta), device_id_type=mesh_id)
    others = [x_peer(1), x_peer(2), x_peer(3), mate] + [{"fsdp": ((x + d) % 4) * 2 + 1 - core} for d in (1, 2, 3)]
    for device in others:
        pl.semaphore_signal(barrier, inc=1, device_id=device, device_id_type=mesh_id)
    pl.semaphore_wait(barrier, 11)

    started = {}
    mates = []

    def send(key, device, pairs, n):
        copies = []
        for arr, (src, dst) in enumerate(pairs):
            copy = pltpu.make_async_remote_copy(
                src_ref=src, dst_ref=dst, send_sem=send_sem.at[arr, n], recv_sem=recv_sem.at[arr, n],
                device_id=device, device_id_type=mesh_id)
            copy.start()
            copies.append(copy)
        started[key] = copies

    def got(key):
        for copy in started[key]:
            copy.wait_recv()

    def piece(zz, yy, q, k):
        return gu_out.at[:, zz, yy, q, k], dn_out.at[zz, yy, q, k]

    def to_mate(refs):
        n = len(mates)
        copies = []
        for arr, ref in enumerate(refs):
            copy = pltpu.make_async_remote_copy(
                src_ref=ref, dst_ref=ref, send_sem=mate_send.at[arr, n], recv_sem=mate_recv.at[arr, n],
                device_id=mate, device_id_type=mesh_id)
            copy.start()
            copies.append(copy)
        mates.append(copies)

    here = piece(z, y, x, core)
    for d in (1, 3, 2):
        send(("x", d), x_peer(d), tuple(zip((gu_ref, dn_ref), here)), d - 1)
    most = []
    for n, device in enumerate(others):
        copy = pltpu.make_async_remote_copy(
            src_ref=most_ref, dst_ref=most_out.at[f], send_sem=most_send.at[n], recv_sem=most_recv.at[n],
            device_id=device, device_id_type=mesh_id)
        copy.start()
        most.append(copy)
    most_out[f] = most_ref[...]
    gu_out[:, z, y, x, core] = gu_ref[...]
    dn_out[z, y, x, core] = dn_ref[...]
    for d in (1, 3, 2):
        got(("x", d))

    def forward(c, h, op, d1, d2, dim, delta):
        zz, yy = shifted2(c, d1, d2)
        refs = piece(zz, yy, 2 * c + h, core)
        send((c, h, op), plane_device(c, dim, delta), tuple(zip(refs, refs)), 3 + 15 * (2 * c + h) + op)

    def arrived(c, h, op, d1, d2):
        got((c, h, op))
        zz, yy = shifted2(c, d1, d2)
        to_mate(piece(zz, yy, 2 * c + h, core))

    quarters = tuple((c, h) for h in (0, 1) for c in (0, 1))
    sides = ((0, -1), (1, 1))
    for c, h in quarters:
        for k, side in sides:
            forward(c, h, k, 0, 0, 0, -side)
        for k, side in sides:
            forward(c, h, 3 + k, 0, 0, 1, -side)
    for c, h in quarters:
        to_mate(piece(z, y, 2 * c + h, core))
    for k, side in sides:
        for c, h in quarters:
            arrived(c, h, k, side, 0)
            if h == k:
                forward(c, h, 2, side, 0, 0, -side)
            for j, out in sides:
                forward(c, h, 5 + 2 * k + j, side, 0, 1, -out)
    for k, side in sides:
        for c, h in quarters:
            arrived(c, h, 3 + k, 0, side)
            if h == k:
                forward(c, h, 11, 0, side, 1, -side)
    for c, h in quarters:
        arrived(c, h, 2, 2, 0)
        for j, out in sides:
            forward(c, h, 9 + j, 2, 0, 1, -out)
    for s, col in sides:
        for k, side in sides:
            for c, h in quarters:
                arrived(c, h, 5 + 2 * s + k, col, side)
                if h == k:
                    forward(c, h, 12 + s, col, side, 1, -side)
    for c, h in quarters:
        arrived(c, h, 11, 0, 2)
    for k, side in sides:
        for c, h in quarters:
            arrived(c, h, 9 + k, 2, side)
            if h == k:
                forward(c, h, 14, 2, side, 1, -side)
    for s, col in sides:
        for c, h in quarters:
            arrived(c, h, 12 + s, col, 2)
    for c, h in quarters:
        arrived(c, h, 14, 2, 2)
    for copies in mates + [most]:
        for copy in copies:
            copy.wait_recv()
    for copies in list(started.values()) + mates + [most]:
        for copy in copies:
            copy.wait_send()


def gather_weights(gate_up, down, most, collective_id):
    _, rows, feats = gate_up.shape
    sl, width = down.shape
    side = (MODEL_SIDE, MODEL_SIDE, 4, 2)
    vmem = pl.BlockSpec(memory_space=pltpu.VMEM)
    gu, dn, most = pl.pallas_call(
        weights_kernel,
        out_shape=(
            jax.ShapeDtypeStruct((2,) + side + (rows, feats), BF16),
            jax.ShapeDtypeStruct(side + (sl, width), BF16),
            jax.ShapeDtypeStruct((8, 8, 128), jnp.int32),
        ),
        in_specs=[vmem, vmem, vmem],
        out_specs=(vmem, vmem, vmem),
        scratch_shapes=[
            pltpu.SemaphoreType.DMA((2, 63)),
            pltpu.SemaphoreType.DMA((2, 63)),
            pltpu.SemaphoreType.DMA((2, 64)),
            pltpu.SemaphoreType.DMA((2, 64)),
            pltpu.SemaphoreType.DMA((7,)),
            pltpu.SemaphoreType.DMA((7,)),
        ],
        compiler_params=pltpu.CompilerParams(collective_id=collective_id, has_side_effects=True),
        cost_estimate=pl.CostEstimate(flops=12_000_000_000, bytes_accessed=10_000_000, transcendentals=0),
    )(gate_up, down, jnp.broadcast_to(most, (8, 128)))
    n_model = MODEL_SIDE * MODEL_SIDE
    return gu.reshape(2, n_model, 8 * rows, feats), dn.reshape(n_model, 8 * sl, width), jnp.max(most)


def solution(mesh):
    n_model, n_fsdp = mesh.shape["model"], mesh.shape["fsdp"]
    tok_spec = P("fsdp", None)
    row_spec = P(("model", "fsdp"), None)
    weight_spec = P("fsdp", None)

    def device_step(tok_ids, tok_labels, table_shard, gate_shard, up_shard, down_shard, gain_in, gain_out):
        me = lax.axis_index("model")
        group = tok_ids.shape[0] * tok_ids.shape[1]
        num_tokens = group * n_fsdp
        part = group // n_model
        rows, width = table_shard.shape
        pad_rows = -(-rows // 16) * 16
        block = rows * n_fsdp
        pad_block = pad_rows * n_fsdp
        hidden = gate_shard.shape[1]
        wg_rows, wd_rows = gate_shard.shape[0], down_shard.shape[0]
        sl = wd_rows // n_model
        fs = sl * n_fsdp

        table = lax.all_gather(jnp.pad(table_shard, ((0, pad_rows - rows), (0, 0))), "fsdp", axis=0, tiled=True)
        gate_all = gate_shard.reshape(wg_rows, n_fsdp, n_model, sl)
        up_all = up_shard.reshape(wg_rows, n_fsdp, n_model, sl)
        gate_sl = lax.dynamic_index_in_dim(gate_all, me, 2, keepdims=False).reshape(wg_rows, fs)
        up_sl = lax.dynamic_index_in_dim(up_all, me, 2, keepdims=False).reshape(wg_rows, fs)
        down_sl = lax.dynamic_slice_in_dim(down_shard, me * sl, sl, 0)
        cap = part // 4
        ids = tok_ids.reshape(group)
        blk = (ids // block).reshape(n_model, part)
        loc = ids - me * block
        loc = (loc + (pad_rows - rows) * (loc // rows)).reshape(n_model, part)
        p_iota = jnp.arange(part, dtype=jnp.int32)
        m_iota = jnp.arange(n_model, dtype=jnp.int32)
        same = (blk[:, :, None] == blk[:, None, :]) & (p_iota[None, None, :] < p_iota[None, :, None])
        rank = jnp.sum(same.astype(jnp.int32), axis=2)
        cnt = jnp.sum((blk[:, :, None] == m_iota).astype(jnp.int32), axis=1)
        own_cnt = jnp.sum((blk == me).astype(jnp.int32), axis=1)
        w_gu, w_down, most = gather_weights(jnp.stack([gate_sl, up_sl]), down_sl, jnp.max(cnt), 6)
        rounds = (most + cap - 1) // cap
        j_iota = jnp.arange(cap, dtype=jnp.int32)
        my_blk = lax.dynamic_index_in_dim(blk, me, 0, keepdims=False)
        my_rank = lax.dynamic_index_in_dim(rank, me, 0, keepdims=False)

        def slots(k):
            hit = (blk[:, None, :] == me) & (rank[:, None, :] == (j_iota + k * cap)[None, :, None])
            return jnp.sum(jnp.where(hit, loc[:, None, :], 0), axis=2).reshape(n_model * cap)

        def pick(k):
            place = my_blk * cap + my_rank - k * cap
            place = jnp.where((my_rank >= k * cap) & (my_rank < (k + 1) * cap), place, -1)
            return place[:, None] == jnp.arange(n_model * cap, dtype=jnp.int32)[None, :]

        def fetch(k):
            got = lax.all_to_all(jnp.take(table, slots(k), axis=0), "model", 0, 0, tiled=True)
            return dot("ij,jd->id", pick(k).astype(BF16), got)

        def give(k, d_x, base):
            send = jnp.einsum("ij,id->jd", pick(k).astype(F32), d_x, precision=lax.Precision.HIGHEST, preferred_element_type=F32)
            got = lax.all_to_all(send, "model", 0, 0, tiled=True)
            return add_rows(base, got, slots(k), jnp.clip(own_cnt - k * cap, 0, cap), cap)

        x_emb = fetch(0)
        x_emb = lax.while_loop(lambda c: c[0] < rounds, lambda c: (c[0] + 1, c[1] + fetch(c[0])), (jnp.int32(1), x_emb))[1]

        normed_in, norm_in_back = jax.vjp(lambda values: rms_scale(values, gain_in), x_emb)
        a_bf = normed_in.astype(BF16)
        gate_up = dot("td,gmdf->gtmf", a_bf, w_gu).astype(BF16).astype(F32)
        gate_f, up_f = gate_up[0], gate_up[1]
        gate_sig = jax.nn.sigmoid(gate_f)
        silu_gate = gate_f * gate_sig
        act_bf = (silu_gate * up_f).astype(BF16)
        mlp_out = dot("tmf,mfd->td", act_bf, w_down).astype(BF16)
        h_res = x_emb + mlp_out.astype(F32)
        hn_f, norm_out_back = jax.vjp(lambda values: rms_scale(values, gain_out), h_res)
        hn_bf = plane_gather(hn_f.astype(BF16), 1).reshape(group, width)

        a_late = lax.optimization_barrier((a_bf, hn_bf))[0]
        a_all = lax.all_gather(a_late, "model", axis=0, tiled=True)
        wgu_s = lax.dynamic_index_in_dim(w_gu, me, 1, keepdims=False)
        gs_us = dot("td,gdf->gtf", a_all, wgu_s).astype(BF16)

        labels = tok_labels.reshape(group)
        lab = labels - me * block
        lab_in = (lab >= 0) & (lab < block)
        lab = jnp.where(lab_in, lab + (pad_rows - rows) * (lab // rows), -1)
        row = lax.broadcasted_iota(jnp.int32, (pad_block, group), 0)
        logits = dot("vd,td->vt", table, hn_bf)
        logits = jnp.where(row % pad_rows < rows, logits, -jnp.inf)
        loc_max = jnp.max(logits, axis=0)
        loc_sum = jnp.sum(jnp.exp(logits - loc_max), axis=0)
        onehot = row == lab
        loc_lab = jnp.sum(jnp.where(onehot, logits, 0.0), axis=0)
        row_max, sum_exp, lab_logit = stats_exchange(jnp.stack([loc_max, loc_sum, loc_lab]), 2)
        tok_loss = row_max + jnp.log(sum_exp) - lab_logit
        loss_part = jnp.sum(tok_loss)
        soft = jnp.exp(logits - row_max) / sum_exp
        d_logits = (jnp.where(onehot, soft - 1.0, soft) / num_tokens).astype(BF16)
        dhn_part = dot("vt,vd->td", d_logits, table).reshape(n_model, part, width)
        dhn_part, gs_us = lax.optimization_barrier((dhn_part, gs_us))
        d_hn, d_head = plane_scatter(dhn_part, d_logits, hn_bf, 3)

        d_hidden = norm_out_back(d_hn)[0]
        d_mlp = d_hidden.astype(BF16)
        dm_all = plane_gather(d_mlp, 4).reshape(group, width)
        wd_s = lax.dynamic_index_in_dim(w_down, me, 0, keepdims=False)
        gs, us = gs_us[0].astype(F32), gs_us[1].astype(F32)
        sig_s = jax.nn.sigmoid(gs)
        silu_s = gs * sig_s
        act_s = (silu_s * us).astype(BF16)
        d_act_s = dot("td,fd->tf", dm_all, wd_s)
        d_gate_s = (d_act_s * us * (sig_s * (1.0 + gs * (1.0 - sig_s)))).astype(BF16)
        d_up_s = (d_act_s * silu_s).astype(BF16)
        gg = dot("td,tf->df", a_all, d_gate_s).reshape(n_fsdp, wg_rows, fs)
        gu = dot("td,tf->df", a_all, d_up_s).reshape(n_fsdp, wg_rows, fs)
        gd = dot("tf,td->fd", act_s, dm_all).reshape(n_fsdp, wg_rows, fs)
        gl = jnp.full((n_fsdp, 16, fs), loss_part)
        cat = jnp.concatenate([gg, gu, gd, gl], 1).reshape(-1, fs)
        cat, d_mlp, d_hidden = lax.optimization_barrier((cat, d_mlp, d_hidden))
        d_act = dot("td,mfd->tmf", d_mlp, w_down)
        silu_back = gate_sig * (1.0 + gate_f * (1.0 - gate_sig))
        d_gate = (d_act * up_f * silu_back).astype(BF16)
        d_up = (d_act * silu_gate).astype(BF16)
        d_normed = dot("gtmf,gmdf->td", jnp.stack([d_gate, d_up]), w_gu)
        d_x = d_hidden + norm_in_back(d_normed)[0]
        grad_block = give(0, d_x, d_head)
        grad_block = lax.while_loop(lambda c: c[0] < rounds, lambda c: (c[0] + 1, give(c[0], d_x, c[1])), (jnp.int32(1), grad_block))[1]
        grad_table = lax.psum_scatter(grad_block, "fsdp", scatter_dimension=0, tiled=True)[:rows]

        cat = lax.psum_scatter(cat, "fsdp", scatter_dimension=0, tiled=True)
        loss = cat[3 * wg_rows, 0] / num_tokens
        cat = plane_gather(cat[: 3 * wg_rows], 5).reshape(n_model, 3, wg_rows, fs)
        grad_gate = cat[:, 0].reshape(n_model, wg_rows, n_fsdp, sl).transpose(1, 2, 0, 3).reshape(wg_rows, hidden)
        grad_up = cat[:, 1].reshape(n_model, wg_rows, n_fsdp, sl).transpose(1, 2, 0, 3).reshape(wg_rows, hidden)
        grad_down = cat[:, 2].reshape(wd_rows, width)
        return loss, grad_table, grad_gate, grad_up, grad_down

    return jax.shard_map(device_step, mesh=mesh, in_specs=(tok_spec, tok_spec, row_spec, weight_spec, weight_spec, weight_spec, P(), P()), out_specs=(P(), row_spec, weight_spec, weight_spec, weight_spec), check_vma=False)
```

```python
import functools

import jax
import jax.numpy as jnp
from jax import lax
from jax.experimental import pallas as pl
from jax.experimental.pallas import tpu as pltpu
from jax.sharding import PartitionSpec as P

EPS = 1e-6
F32 = jnp.float32
BF16 = jnp.bfloat16


def rms_scale(values, gain_vec):
    mean_sq = jnp.mean(values * values, axis=-1, keepdims=True)
    return values * lax.rsqrt(mean_sq + EPS) * gain_vec


def dot(spec, lhs, rhs):
    return jnp.einsum(spec, lhs, rhs, preferred_element_type=F32)


def rounded(values):
    return lax.reduce_precision(values, 8, 7)


def add_rows_kernel(cap, count_ref, row_ref, add_ref, base_ref, out_ref):
    out_ref[...] = base_ref[...]

    def chunk(c, carry):
        def step(j, carry):
            row = row_ref[c * cap + j]
            out_ref[pl.ds(row, 1), :] += add_ref[pl.ds(c * cap + j, 1), :]
            return carry

        return lax.fori_loop(0, count_ref[c], step, carry)

    lax.fori_loop(0, count_ref.shape[0], chunk, 0)


def add_rows(base, rows, row_ids, counts, cap):
    vmem = pl.BlockSpec(memory_space=pltpu.VMEM)
    smem = pl.BlockSpec(memory_space=pltpu.SMEM)
    return pl.pallas_call(
        functools.partial(add_rows_kernel, cap),
        out_shape=jax.ShapeDtypeStruct(base.shape, base.dtype),
        in_specs=[smem, smem, vmem, vmem],
        out_specs=vmem,
        cost_estimate=pl.CostEstimate(flops=1_500_000_000, bytes_accessed=20_000_000, transcendentals=0),
    )(counts, row_ids, rows, base)


MODEL_SIDE = 4


def plane_coords():
    me = lax.axis_index("model")
    return me // MODEL_SIDE, me % MODEL_SIDE


def shifted(color, dim, delta):
    z, y = plane_coords()
    if (color == 0) == (dim == 0):
        y = (y + delta + MODEL_SIDE) % MODEL_SIDE
    else:
        z = (z + delta + MODEL_SIDE) % MODEL_SIDE
    return z, y


def shifted2(color, delta1, delta2):
    z, y = plane_coords()
    if color == 0:
        return (z + delta2 + MODEL_SIDE) % MODEL_SIDE, (y + delta1 + MODEL_SIDE) % MODEL_SIDE
    return (z + delta1 + MODEL_SIDE) % MODEL_SIDE, (y + delta2 + MODEL_SIDE) % MODEL_SIDE


def plane_device(color, dim, delta):
    z, y = shifted(color, dim, delta)
    return {"model": z * MODEL_SIDE + y}


def greet_plane():
    barrier = pltpu.get_barrier_semaphore()
    for dim in (0, 1):
        for delta in (1, -1):
            pl.semaphore_signal(barrier, inc=1, device_id=plane_device(0, dim, delta), device_id_type=pl.DeviceIdType.MESH)
    pl.semaphore_wait(barrier, 4)


GATHER_OPS = 22


def plane_gather_kernel(x_ref, out_ref, send_sem, recv_sem):
    z, y = plane_coords()
    greet_plane()
    started = {}

    def send(color, op, dim, delta, src, dst):
        copy = pltpu.make_async_remote_copy(
            src_ref=src, dst_ref=dst, send_sem=send_sem.at[color, op], recv_sem=recv_sem.at[color, op],
            device_id=plane_device(color, dim, delta), device_id_type=pl.DeviceIdType.MESH)
        copy.start()
        started[color, op] = copy

    def got(color, op):
        started[color, op].wait_recv()

    def block(color, d1, d2):
        zz, yy = shifted2(color, d1, d2)
        return out_ref.at[zz, yy, color]

    def half(color, d1, d2, h):
        zz, yy = shifted2(color, d1, d2)
        return out_ref.at[zz, yy, color, h]

    colors = (0, 1)
    for c in colors:
        for k, delta in enumerate((1, -1)):
            send(c, k, 0, delta, x_ref.at[c], block(c, 0, 0))
        for k, delta in enumerate((1, -1)):
            send(c, 4 + k, 1, delta, x_ref.at[c], block(c, 0, 0))
    out_ref[z, y] = x_ref[...]
    for k in (0, 1):
        side = -1 if k == 0 else 1
        for c in colors:
            got(c, k)
            send(c, 2 + k, 0, -side, half(c, side, 0, k), half(c, side, 0, k))
            for j, delta in enumerate((1, -1)):
                send(c, 6 + 2 * k + j, 1, delta, block(c, side, 0), block(c, side, 0))
    for k in (0, 1):
        side = -1 if k == 0 else 1
        for c in colors:
            got(c, 4 + k)
            send(c, 14 + k, 1, -side, half(c, 0, side, k), half(c, 0, side, k))
    for k in (0, 1):
        for c in colors:
            got(c, 2 + k)
            for j, delta in enumerate((1, -1)):
                send(c, 10 + 2 * k + j, 1, delta, half(c, 2, 0, k), half(c, 2, 0, k))
    for s, col in ((0, -1), (1, 1)):
        for k in (0, 1):
            side = -1 if k == 0 else 1
            for c in colors:
                got(c, 6 + 2 * s + k)
                send(c, 16 + 2 * s + k, 1, -side, half(c, col, side, k), half(c, col, side, k))
    for k in (0, 1):
        side = -1 if k == 0 else 1
        for c in colors:
            got(c, 10 + 2 * k + k)
            send(c, 20 + k, 1, -side, half(c, 2, side, k), half(c, 2, side, k))
    for c in colors:
        got(c, 11)
        got(c, 12)
        for op in range(14, GATHER_OPS):
            got(c, op)
    for copy in started.values():
        copy.wait_send()


def plane_gather(x, collective_id):
    rows, width = x.shape
    quarter = rows // 4
    vmem = pl.BlockSpec(memory_space=pltpu.VMEM)
    out = pl.pallas_call(
        plane_gather_kernel,
        out_shape=jax.ShapeDtypeStruct((MODEL_SIDE, MODEL_SIDE, 2, 2, quarter, width), x.dtype),
        in_specs=[vmem],
        out_specs=vmem,
        scratch_shapes=[pltpu.SemaphoreType.DMA((2, GATHER_OPS)), pltpu.SemaphoreType.DMA((2, GATHER_OPS))],
        compiler_params=pltpu.CompilerParams(collective_id=collective_id, has_side_effects=True),
        cost_estimate=pl.CostEstimate(flops=5_000_000_000, bytes_accessed=4_000_000, transcendentals=0),
    )(x.reshape(2, 2, quarter, width))
    return out.reshape(MODEL_SIDE * MODEL_SIDE, rows, width)


def plane_scatter_kernel(x_ref, dz_ref, hn_ref, out_ref, head_ref, far1, near1, relay1, sum1, far2, near2, relay2, dz_buf, hn_buf, head_buf, send_sem, recv_sem, dz_sem, hn_sem, head_sem):
    greet_plane()
    started = []
    hn_copy = pltpu.make_async_copy(hn_ref, hn_buf, hn_sem)
    n_blocks = dz_ref.shape[0]
    dz_copies = [pltpu.make_async_copy(dz_ref.at[i], dz_buf.at[i], dz_sem.at[i]) for i in range(n_blocks)]
    head_copies = []

    def head_block():
        i = len(head_copies)
        if i == 0:
            hn_copy.wait()
        dz_copies[i].wait()
        head_buf[i] = jnp.dot(dz_buf[i], hn_buf[...], preferred_element_type=F32)
        copy = pltpu.make_async_copy(head_buf.at[i], head_ref.at[i], head_sem.at[i])
        copy.start()
        head_copies.append(copy)


    def send(color, op, dim, delta, src, dst):
        copy = pltpu.make_async_remote_copy(
            src_ref=src, dst_ref=dst, send_sem=send_sem.at[color, op], recv_sem=recv_sem.at[color, op],
            device_id=plane_device(color, dim, delta), device_id_type=pl.DeviceIdType.MESH)
        copy.start()
        started.append(copy)
        return copy

    def mine(color, d1, d2, h):
        zz, yy = shifted2(color, d1, d2)
        return x_ref.at[zz, yy, color, h]

    colors = (0, 1)
    order = (2, 1, -1, 0)
    sides = ((0, 1), (1, -1))
    copies = {}
    for n, d2 in enumerate(order):
        for c in colors:
            for k, delta in sides:
                copies[c, n, k] = send(c, 2 * n + k, 0, delta, mine(c, 2, d2, k), far1.at[c, n, k])
    hn_copy.start()
    for copy in dz_copies:
        copy.start()
    for n, d2 in enumerate(order):
        for c in colors:
            for k, delta in sides:
                copies[c, n, 2 + k] = send(c, 8 + 2 * n + k, 0, delta, mine(c, delta, d2, 1 - k), near1.at[c, n, k, 0])
        for c in colors:
            for k, delta in sides:
                copies[c, n, k].wait_recv()
                relay1[c, n, k] = far1[c, n, k] + mine(c, delta, d2, k)[...]
                copies[c, n, 4 + k] = send(c, 16 + 2 * n + k, 0, delta, relay1.at[c, n, k], near1.at[c, n, k, 1])
        head_block()
    for n, d2 in enumerate(order):
        head_block()
        for c in colors:
            for k in (2, 3, 4, 5):
                copies[c, n, k].wait_recv()
            for h in (0, 1):
                sum1[c, n, h] = mine(c, 0, d2, h)[...] + near1[c, n, h, 1] + near1[c, n, 1 - h, 0]
            if n == 0:
                for k, delta in sides:
                    copies[c, "far", k] = send(c, 24 + k, 1, delta, sum1.at[c, 0, k], far2.at[c, k])
            if n in (1, 2):
                k, delta = sides[n - 1]
                copies[c, "raw", k] = send(c, 26 + k, 1, delta, sum1.at[c, n, 1 - k], near2.at[c, k, 0])
                copies[c, "far", k].wait_recv()
                relay2[c, k] = far2[c, k] + sum1[c, n, k]
                copies[c, "sum", k] = send(c, 28 + k, 1, delta, relay2.at[c, k], near2.at[c, k, 1])
    for c in colors:
        for k in (0, 1):
            copies[c, "raw", k].wait_recv()
            copies[c, "sum", k].wait_recv()
        for h in (0, 1):
            out_ref[c, h] = sum1[c, 3, h] + near2[c, h, 1] + near2[c, 1 - h, 0]
    while len(head_copies) < n_blocks:
        head_block()
    for copy in started:
        copy.wait_send()
    for copy in head_copies:
        copy.wait()


def plane_scatter(x, dz, hn, collective_id):
    _, rows, width = x.shape
    n_blocks = 8
    vocab, tokens = dz.shape
    block_rows = vocab // n_blocks
    any_space = pl.BlockSpec(memory_space=pl.ANY)
    quarter = rows // 4
    vmem = pl.BlockSpec(memory_space=pltpu.VMEM)
    piece = (quarter, width)
    out, head = pl.pallas_call(
        plane_scatter_kernel,
        out_shape=(jax.ShapeDtypeStruct((2, 2, quarter, width), F32), jax.ShapeDtypeStruct((n_blocks, block_rows, width), F32)),
        in_specs=[vmem, any_space, any_space],
        out_specs=(vmem, any_space),
        scratch_shapes=[
            pltpu.VMEM((2, 4, 2) + piece, F32),
            pltpu.VMEM((2, 4, 2, 2) + piece, F32),
            pltpu.VMEM((2, 4, 2) + piece, F32),
            pltpu.VMEM((2, 4, 2) + piece, F32),
            pltpu.VMEM((2, 2) + piece, F32),
            pltpu.VMEM((2, 2, 2) + piece, F32),
            pltpu.VMEM((2, 2) + piece, F32),
            pltpu.VMEM((n_blocks, block_rows, tokens), BF16),
            pltpu.VMEM((tokens, width), BF16),
            pltpu.VMEM((n_blocks, block_rows, width), F32),
            pltpu.SemaphoreType.DMA((2, 30)),
            pltpu.SemaphoreType.DMA((2, 30)),
            pltpu.SemaphoreType.DMA((n_blocks,)),
            pltpu.SemaphoreType.DMA(()),
            pltpu.SemaphoreType.DMA((n_blocks,)),
        ],
        compiler_params=pltpu.CompilerParams(collective_id=collective_id, has_side_effects=True),
        cost_estimate=pl.CostEstimate(flops=10_000_000_000, bytes_accessed=8_000_000, transcendentals=0),
    )(x.reshape(MODEL_SIDE, MODEL_SIDE, 2, 2, quarter, width), dz.reshape(n_blocks, block_rows, tokens), hn)
    return out.reshape(rows, width), head.reshape(vocab, width)


def stats_kernel(x_ref, out_ref, buf1, comb, buf2, send_sem, recv_sem):
    z, y = plane_coords()

    def peer(dim, d):
        zz, yy = (z, (y + d) % MODEL_SIDE) if dim == 0 else ((z + d) % MODEL_SIDE, y)
        return {"model": zz * MODEL_SIDE + yy}

    barrier = pltpu.get_barrier_semaphore()
    for dim in (0, 1):
        for d in (1, 2, 3):
            pl.semaphore_signal(barrier, inc=1, device_id=peer(dim, d), device_id_type=pl.DeviceIdType.MESH)
    pl.semaphore_wait(barrier, 6)

    def merged(buf):
        top = jnp.maximum(jnp.maximum(buf[0, 0], buf[1, 0]), jnp.maximum(buf[2, 0], buf[3, 0]))
        total = jnp.zeros_like(top)
        label = jnp.zeros_like(top)
        for k in range(MODEL_SIDE):
            total = total + buf[k, 1] * jnp.exp(buf[k, 0] - top)
            label = label + buf[k, 2]
        return top, total, label

    for dim, src, buf, place, dst in ((0, x_ref, buf1, y, comb), (1, comb, buf2, z, out_ref)):
        copies = []
        for d in (1, 2, 3):
            copy = pltpu.make_async_remote_copy(
                src_ref=src, dst_ref=buf.at[place], send_sem=send_sem.at[dim, d - 1], recv_sem=recv_sem.at[dim, d - 1],
                device_id=peer(dim, d), device_id_type=pl.DeviceIdType.MESH)
            copy.start()
            copies.append(copy)
        buf[place] = src[...]
        for copy in copies:
            copy.wait_recv()
        top, total, label = merged(buf)
        dst[0] = top
        dst[1] = total
        dst[2] = label
        for copy in copies:
            copy.wait_send()


def stats_exchange(stats, collective_id):
    rows = stats.shape[1] // 128
    vmem = pl.BlockSpec(memory_space=pltpu.VMEM)
    out = pl.pallas_call(
        stats_kernel,
        out_shape=jax.ShapeDtypeStruct((3, rows, 128), F32),
        in_specs=[vmem],
        out_specs=vmem,
        scratch_shapes=[
            pltpu.VMEM((MODEL_SIDE, 3, rows, 128), F32),
            pltpu.VMEM((3, rows, 128), F32),
            pltpu.VMEM((MODEL_SIDE, 3, rows, 128), F32),
            pltpu.SemaphoreType.DMA((2, 3)),
            pltpu.SemaphoreType.DMA((2, 3)),
        ],
        compiler_params=pltpu.CompilerParams(collective_id=collective_id, has_side_effects=True),
        cost_estimate=pl.CostEstimate(flops=2_500_000_000, bytes_accessed=400_000, transcendentals=0),
    )(stats.reshape(3, rows, 128))
    return out.reshape(3, rows * 128)


def start_kernel(
    gu_ref, dn_ref, most_ref, table_ref, slot_ref, place_ref, gu_out, dn_out, most_out, table_out, x_out, emb_send, emb_got,
    send_sem, recv_sem, mate_send, mate_recv, most_send, most_recv, row_send, row_recv, emb_send_sem, emb_recv_sem,
):
    z, y = plane_coords()
    me = lax.axis_index("model")
    f = lax.axis_index("fsdp")
    x, core = f // 2, f % 2
    mesh_id = pl.DeviceIdType.MESH
    n_model, cap, width = emb_send.shape
    pad_rows = table_ref.shape[0]

    def x_peer(d):
        return {"fsdp": ((x + d) % 4) * 2 + core}

    def plane_peer(d):
        return {"model": (me + d) % n_model}

    mate = {"fsdp": x * 2 + 1 - core}
    barrier = pltpu.get_barrier_semaphore()
    others = [x_peer(1), x_peer(2), x_peer(3), mate] + [{"fsdp": ((x + d) % 4) * 2 + 1 - core} for d in (1, 2, 3)]
    for device in others + [plane_peer(d) for d in range(1, n_model)]:
        pl.semaphore_signal(barrier, inc=1, device_id=device, device_id_type=mesh_id)
    pl.semaphore_wait(barrier, len(others) + n_model - 1)

    started = {}
    mates = []

    def send(key, device, pairs, n):
        copies = []
        for arr, (src, dst) in enumerate(pairs):
            copy = pltpu.make_async_remote_copy(
                src_ref=src, dst_ref=dst, send_sem=send_sem.at[arr, n], recv_sem=recv_sem.at[arr, n],
                device_id=device, device_id_type=mesh_id)
            copy.start()
            copies.append(copy)
        started[key] = copies

    def got(key):
        for copy in started[key]:
            copy.wait_recv()

    def piece(zz, yy, q, k):
        return gu_out.at[:, zz, yy, q, k], dn_out.at[zz, yy, q, k]

    def to_mate(refs):
        n = len(mates)
        copies = []
        for arr, ref in enumerate(refs):
            copy = pltpu.make_async_remote_copy(
                src_ref=ref, dst_ref=ref, send_sem=mate_send.at[arr, n], recv_sem=mate_recv.at[arr, n],
                device_id=mate, device_id_type=mesh_id)
            copy.start()
            copies.append(copy)
        mates.append(copies)

    row_copies = {}

    def table_rows(d, h, kind):
        start = (((x + d) % 4) * 2 + kind) * pad_rows
        if h is None:
            return table_out.at[pl.ds(pl.multiple_of(start, 16), pad_rows), :]
        return table_out.at[pl.ds(pl.multiple_of(start + h * (pad_rows // 2), 16), pad_rows // 2), :]

    def send_rows(n, device, src, dst):
        copy = pltpu.make_async_remote_copy(
            src_ref=src, dst_ref=dst, send_sem=row_send.at[n], recv_sem=row_recv.at[n], device_id=device, device_id_type=mesh_id)
        copy.start()
        row_copies[n] = copy

    def relay_rows(n, device, d, h):
        rows = table_rows(d, h, core)
        send_rows(n, device, rows, rows)

    here = piece(z, y, x, core)
    for d in (1, 3, 2):
        send(("x", d), x_peer(d), tuple(zip((gu_ref, dn_ref), here)), d - 1)
    most = []
    for n, device in enumerate(others):
        copy = pltpu.make_async_remote_copy(
            src_ref=most_ref, dst_ref=most_out.at[f], send_sem=most_send.at[n], recv_sem=most_recv.at[n],
            device_id=device, device_id_type=mesh_id)
        copy.start()
        most.append(copy)
    send_rows(0, x_peer(1), table_ref, table_rows(0, None, core))
    send_rows(1, x_peer(3), table_ref, table_rows(0, None, core))
    send_rows(4, mate, table_ref, table_rows(0, None, core))
    most_out[f] = most_ref[...]
    table_out[pl.ds(pl.multiple_of((x * 2 + core) * pad_rows, 16), pad_rows), :] = table_ref[...]
    gu_out[:, z, y, x, core] = gu_ref[...]
    dn_out[z, y, x, core] = dn_ref[...]
    for d in (1, 3, 2):
        got(("x", d))

    def forward(c, h, op, d1, d2, dim, delta):
        zz, yy = shifted2(c, d1, d2)
        refs = piece(zz, yy, 2 * c + h, core)
        send((c, h, op), plane_device(c, dim, delta), tuple(zip(refs, refs)), 3 + 15 * (2 * c + h) + op)

    def arrived(c, h, op, d1, d2):
        got((c, h, op))
        zz, yy = shifted2(c, d1, d2)
        to_mate(piece(zz, yy, 2 * c + h, core))

    quarters = tuple((c, h) for h in (0, 1) for c in (0, 1))
    sides = ((0, -1), (1, 1))
    for c, h in quarters:
        for k, side in sides:
            forward(c, h, k, 0, 0, 0, -side)
        for k, side in sides:
            forward(c, h, 3 + k, 0, 0, 1, -side)
    for c, h in quarters:
        to_mate(piece(z, y, 2 * c + h, core))
    for k, side in sides:
        for c, h in quarters:
            arrived(c, h, k, side, 0)
            if h == k:
                forward(c, h, 2, side, 0, 0, -side)
            for j, out in sides:
                forward(c, h, 5 + 2 * k + j, side, 0, 1, -out)
    for k, side in sides:
        row_copies[k].wait_recv()
        relay_rows(2 + k, x_peer(-side), side, k)
        relay_rows(5 + k, mate, side, None)
    for k, side in sides:
        for c, h in quarters:
            arrived(c, h, 3 + k, 0, side)
            if h == k:
                forward(c, h, 11, 0, side, 1, -side)
    for c, h in quarters:
        arrived(c, h, 2, 2, 0)
        for j, out in sides:
            forward(c, h, 9 + j, 2, 0, 1, -out)
    for k, side in sides:
        row_copies[2 + k].wait_recv()
        relay_rows(7 + k, mate, 2, k)
    for n in (4, 5, 6, 7, 8):
        row_copies[n].wait_recv()
    emb_copies = []
    step = n_model * cap // 4
    for n in range(4):
        hit = slot_ref[n * step : (n + 1) * step, :] == lax.broadcasted_iota(jnp.int32, (step, table_out.shape[0]), 1)
        got_rows = jnp.dot(hit.astype(F32).astype(BF16), table_out[...], preferred_element_type=F32)
        emb_send[n * 4 : (n + 1) * 4] = got_rows.astype(BF16).reshape(4, cap, width)
    for d in range(1, n_model):
        copy = pltpu.make_async_remote_copy(
            src_ref=emb_send.at[(me + d) % n_model], dst_ref=emb_got.at[me], send_sem=emb_send_sem.at[d - 1], recv_sem=emb_recv_sem.at[d - 1],
            device_id=plane_peer(d), device_id_type=mesh_id)
        copy.start()
        emb_copies.append(copy)
    emb_got[me] = emb_send[me]
    for s, col in sides:
        for k, side in sides:
            for c, h in quarters:
                arrived(c, h, 5 + 2 * s + k, col, side)
                if h == k:
                    forward(c, h, 12 + s, col, side, 1, -side)
    for c, h in quarters:
        arrived(c, h, 11, 0, 2)
    for k, side in sides:
        for c, h in quarters:
            arrived(c, h, 9 + k, 2, side)
            if h == k:
                forward(c, h, 14, 2, side, 1, -side)
    for s, col in sides:
        for c, h in quarters:
            arrived(c, h, 12 + s, col, 2)
    for c, h in quarters:
        arrived(c, h, 14, 2, 2)
    for copy in emb_copies:
        copy.wait_recv()
    chosen = place_ref[...] == lax.broadcasted_iota(jnp.int32, (place_ref.shape[0], n_model * cap), 1)
    x_out[...] = jnp.dot(chosen.astype(F32).astype(BF16), emb_got[...].reshape(n_model * cap, width), preferred_element_type=F32)
    for copies in mates + [most]:
        for copy in copies:
            copy.wait_recv()
    for copies in list(started.values()) + mates + [most, list(row_copies.values()), emb_copies]:
        for copy in copies:
            copy.wait_send()


def start_exchange(gate_up, down, most, table, slots, places, cap, collective_id):
    _, rows, feats = gate_up.shape
    sl, width = down.shape
    side = (MODEL_SIDE, MODEL_SIDE, 4, 2)
    n_model = MODEL_SIDE * MODEL_SIDE
    vmem = pl.BlockSpec(memory_space=pltpu.VMEM)
    sems = [(2, 63), (2, 63), (2, 64), (2, 64), (7,), (7,), (9,), (9,), (n_model - 1,), (n_model - 1,)]
    gu, dn, most, table, x_emb = pl.pallas_call(
        start_kernel,
        out_shape=(
            jax.ShapeDtypeStruct((2,) + side + (rows, feats), BF16),
            jax.ShapeDtypeStruct(side + (sl, width), BF16),
            jax.ShapeDtypeStruct((8, 8, 128), jnp.int32),
            jax.ShapeDtypeStruct((8 * table.shape[0], width), BF16),
            jax.ShapeDtypeStruct((places.shape[0], width), F32),
        ),
        in_specs=[vmem] * 6,
        out_specs=(vmem,) * 5,
        scratch_shapes=[pltpu.VMEM((n_model, cap, width), BF16), pltpu.VMEM((n_model, cap, width), BF16)] + [pltpu.SemaphoreType.DMA(n) for n in sems],
        compiler_params=pltpu.CompilerParams(collective_id=collective_id, has_side_effects=True),
        cost_estimate=pl.CostEstimate(flops=12_000_000_000, bytes_accessed=10_000_000, transcendentals=0),
    )(gate_up, down, jnp.broadcast_to(most, (8, 128)), table, slots[:, None], places[:, None])
    return gu.reshape(2, n_model, 8 * rows, feats), dn.reshape(n_model, 8 * sl, width), jnp.max(most), table, x_emb


def solution(mesh):
    n_model, n_fsdp = mesh.shape["model"], mesh.shape["fsdp"]
    tok_spec = P("fsdp", None)
    row_spec = P(("model", "fsdp"), None)
    weight_spec = P("fsdp", None)

    def device_step(tok_ids, tok_labels, table_shard, gate_shard, up_shard, down_shard, gain_in, gain_out):
        me = lax.axis_index("model")
        group = tok_ids.shape[0] * tok_ids.shape[1]
        num_tokens = group * n_fsdp
        part = group // n_model
        rows, width = table_shard.shape
        pad_rows = -(-rows // 16) * 16
        block = rows * n_fsdp
        pad_block = pad_rows * n_fsdp
        hidden = gate_shard.shape[1]
        wg_rows, wd_rows = gate_shard.shape[0], down_shard.shape[0]
        sl = wd_rows // n_model
        fs = sl * n_fsdp

        gate_all = gate_shard.reshape(wg_rows, n_fsdp, n_model, sl)
        up_all = up_shard.reshape(wg_rows, n_fsdp, n_model, sl)
        gate_sl = lax.dynamic_index_in_dim(gate_all, me, 2, keepdims=False).reshape(wg_rows, fs)
        up_sl = lax.dynamic_index_in_dim(up_all, me, 2, keepdims=False).reshape(wg_rows, fs)
        down_sl = lax.dynamic_slice_in_dim(down_shard, me * sl, sl, 0)
        cap = part // 4
        ids = tok_ids.reshape(group)
        blk = (ids // block).reshape(n_model, part)
        loc = ids - me * block
        loc = (loc + (pad_rows - rows) * (loc // rows)).reshape(n_model, part)
        p_iota = jnp.arange(part, dtype=jnp.int32)
        m_iota = jnp.arange(n_model, dtype=jnp.int32)
        same = (blk[:, :, None] == blk[:, None, :]) & (p_iota[None, None, :] < p_iota[None, :, None])
        rank = jnp.sum(same.astype(jnp.int32), axis=2)
        cnt = jnp.sum((blk[:, :, None] == m_iota).astype(jnp.int32), axis=1)
        own_cnt = jnp.sum((blk == me).astype(jnp.int32), axis=1)
        j_iota = jnp.arange(cap, dtype=jnp.int32)
        my_blk = lax.dynamic_index_in_dim(blk, me, 0, keepdims=False)
        my_rank = lax.dynamic_index_in_dim(rank, me, 0, keepdims=False)

        def slots(k):
            hit = (blk[:, None, :] == me) & (rank[:, None, :] == (j_iota + k * cap)[None, :, None])
            return jnp.sum(jnp.where(hit, loc[:, None, :], 0), axis=2).reshape(n_model * cap)

        def places(k):
            place = my_blk * cap + my_rank - k * cap
            return jnp.where((my_rank >= k * cap) & (my_rank < (k + 1) * cap), place, -1)

        def pick(k):
            return places(k)[:, None] == jnp.arange(n_model * cap, dtype=jnp.int32)[None, :]

        def fetch(k):
            got = lax.all_to_all(jnp.take(table, slots(k), axis=0), "model", 0, 0, tiled=True)
            return dot("ij,jd->id", pick(k).astype(BF16), got)

        def give(k, d_x, base):
            send = jnp.einsum("ij,id->jd", pick(k).astype(F32), d_x, precision=lax.Precision.HIGHEST, preferred_element_type=F32)
            got = lax.all_to_all(send, "model", 0, 0, tiled=True)
            return add_rows(base, got, slots(k), jnp.clip(own_cnt - k * cap, 0, cap), cap)

        shard = jnp.pad(table_shard, ((0, pad_rows - rows), (0, 0)))
        w_gu, w_down, most, table, x_emb = start_exchange(jnp.stack([gate_sl, up_sl]), down_sl, jnp.max(cnt), shard, slots(0), places(0), cap, 6)
        rounds = (most + cap - 1) // cap
        x_emb = lax.while_loop(lambda c: c[0] < rounds, lambda c: (c[0] + 1, c[1] + fetch(c[0])), (jnp.int32(1), x_emb))[1]

        normed_in, norm_in_back = jax.vjp(lambda values: rms_scale(values, gain_in), x_emb)
        a_bf = normed_in.astype(BF16)
        gate_up = rounded(dot("td,gmdf->gtmf", a_bf, w_gu))
        gate_f, up_f = gate_up[0], gate_up[1]
        gate_sig = jax.nn.sigmoid(gate_f)
        silu_gate = gate_f * gate_sig
        act_bf = (silu_gate * up_f).astype(BF16)
        h_res = x_emb + rounded(dot("tmf,mfd->td", act_bf, w_down))
        hn_f, norm_out_back = jax.vjp(lambda values: rms_scale(values, gain_out), h_res)
        hn_bf = plane_gather(hn_f.astype(BF16), 1).reshape(group, width)

        a_late = lax.optimization_barrier((a_bf, hn_bf))[0]
        a_all = lax.all_gather(a_late, "model", axis=0, tiled=True)
        wgu_s = lax.dynamic_index_in_dim(w_gu, me, 1, keepdims=False)
        gs_us = rounded(dot("td,gdf->gtf", a_all, wgu_s))

        labels = tok_labels.reshape(group)
        lab = labels - me * block
        lab_in = (lab >= 0) & (lab < block)
        lab = jnp.where(lab_in, lab + (pad_rows - rows) * (lab // rows), -1)
        row = lax.broadcasted_iota(jnp.int32, (pad_block, group), 0)
        logits = dot("vd,td->vt", table, hn_bf)
        logits = jnp.where(row % pad_rows < rows, logits, -jnp.inf)
        loc_max = jnp.max(logits, axis=0)
        loc_sum = jnp.sum(jnp.exp(logits - loc_max), axis=0)
        onehot = row == lab
        loc_lab = jnp.sum(jnp.where(onehot, logits, 0.0), axis=0)
        row_max, sum_exp, lab_logit = stats_exchange(jnp.stack([loc_max, loc_sum, loc_lab]), 2)
        tok_loss = row_max + jnp.log(sum_exp) - lab_logit
        loss_part = jnp.sum(tok_loss)
        soft = jnp.exp(logits - row_max) / sum_exp
        d_logits = (jnp.where(onehot, soft - 1.0, soft) / num_tokens).astype(BF16)
        dhn_part = dot("vt,vd->td", d_logits, table).reshape(n_model, part, width)
        dhn_part, gs_us = lax.optimization_barrier((dhn_part, gs_us))
        d_hn, d_head = plane_scatter(dhn_part, d_logits, hn_bf, 3)

        d_hidden = norm_out_back(d_hn)[0]
        d_mlp = d_hidden.astype(BF16)
        dm_all = plane_gather(d_mlp, 4).reshape(group, width)
        wd_s = lax.dynamic_index_in_dim(w_down, me, 0, keepdims=False)
        gs, us = gs_us[0], gs_us[1]
        sig_s = jax.nn.sigmoid(gs)
        silu_s = gs * sig_s
        act_s = (silu_s * us).astype(BF16)
        d_act_s = dot("td,fd->tf", dm_all, wd_s)
        d_gate_s = (d_act_s * us * (sig_s * (1.0 + gs * (1.0 - sig_s)))).astype(BF16)
        d_up_s = (d_act_s * silu_s).astype(BF16)
        gg = dot("td,tf->df", a_all, d_gate_s).reshape(n_fsdp, wg_rows, fs)
        gu = dot("td,tf->df", a_all, d_up_s).reshape(n_fsdp, wg_rows, fs)
        gd = dot("tf,td->fd", act_s, dm_all).reshape(n_fsdp, wg_rows, fs)
        gl = jnp.full((n_fsdp, 16, fs), loss_part)
        cat = jnp.concatenate([gg, gu, gd, gl], 1).reshape(-1, fs)
        cat, d_mlp, d_hidden = lax.optimization_barrier((cat, d_mlp, d_hidden))
        d_act = dot("td,mfd->tmf", d_mlp, w_down)
        silu_back = gate_sig * (1.0 + gate_f * (1.0 - gate_sig))
        d_gate = (d_act * up_f * silu_back).astype(BF16)
        d_up = (d_act * silu_gate).astype(BF16)
        d_normed = dot("gtmf,gmdf->td", jnp.stack([d_gate, d_up]), w_gu)
        d_x = d_hidden + norm_in_back(d_normed)[0]
        grad_block = give(0, d_x, d_head)
        grad_block = lax.while_loop(lambda c: c[0] < rounds, lambda c: (c[0] + 1, give(c[0], d_x, c[1])), (jnp.int32(1), grad_block))[1]
        grad_table = lax.psum_scatter(grad_block, "fsdp", scatter_dimension=0, tiled=True)[:rows]

        cat = lax.psum_scatter(cat, "fsdp", scatter_dimension=0, tiled=True)
        loss = cat[3 * wg_rows, 0] / num_tokens
        cat = plane_gather(cat[: 3 * wg_rows], 5).reshape(n_model, 3, wg_rows, fs)
        grad_gate = cat[:, 0].reshape(n_model, wg_rows, n_fsdp, sl).transpose(1, 2, 0, 3).reshape(wg_rows, hidden)
        grad_up = cat[:, 1].reshape(n_model, wg_rows, n_fsdp, sl).transpose(1, 2, 0, 3).reshape(wg_rows, hidden)
        grad_down = cat[:, 2].reshape(wd_rows, width)
        return loss, grad_table, grad_gate, grad_up, grad_down

    return jax.shard_map(device_step, mesh=mesh, in_specs=(tok_spec, tok_spec, row_spec, weight_spec, weight_spec, weight_spec, P(), P()), out_specs=(P(), row_spec, weight_spec, weight_spec, weight_spec), check_vma=False)
```
